32 devices in a mesh: a3: 4 (over z), a2: 2 (over y), a1: 4 (over x, core).
Axes of the slice: x: 2, y: 2, z: 4, core: 2. Of those that a mesh axis runs over, the one named last changes fastest.
Arguments:
- tensor: bfloat16 [384, 720, 1280], P('a1', 'a2', 'a3')
- u_time: float32 [384, 48], replicated
- u_height: float32 [720, 88], replicated
- u_width: float32 [1280, 160], replicated
Outputs:
- output 1: float32 [384, 48], replicated
- output 2: float32 [720, 88], replicated
- output 3: float32 [1280, 160], replicated
- output 4: float32 [48, 88, 160], P('a1', 'a2', 'a3')
- output 5: float32 [], replicated
All inputs are finite; a program needn't handle non-finite values.
Results may differ from the reference program's by a relative error of at most 0.00377637.
Values are sent between devices in bfloat16 or wider.
A program may use at most 1 GiB of HBM per device.

```python
import jax
import jax.numpy as jnp
from jax import lax

FRAMES = 384
GRID_H = 720
GRID_W = 1280
RANK_T = 48
RANK_H = 88
RANK_W = 160
SIGNAL_RANK = 8


def setup_inputs(seed: int = 0) -> dict:
    key_list = jax.random.split(jax.random.key(seed), 8)
    fac_t = jax.random.normal(key_list[0], (FRAMES, SIGNAL_RANK), jnp.float32)
    fac_h = jax.random.normal(key_list[1], (GRID_H, SIGNAL_RANK), jnp.float32)
    fac_w = jax.random.normal(key_list[2], (GRID_W, SIGNAL_RANK), jnp.float32)
    weights = jax.random.uniform(key_list[3], (SIGNAL_RANK,), jnp.float32, 0.5, 1.5) * SIGNAL_RANK ** -0.5

    def one_frame(frame_idx):
        noise_map = jax.random.normal(jax.random.fold_in(key_list[4], frame_idx), (GRID_H, GRID_W), jnp.float32)
        signal = jnp.dot(fac_h * (fac_t[frame_idx] * weights), fac_w.T)
        return (signal + noise_map).astype(jnp.bfloat16)

    tensor = lax.map(one_frame, jnp.arange(FRAMES))
    u_time = jax.random.normal(key_list[5], (FRAMES, RANK_T), jnp.float32) * FRAMES ** -0.5
    u_height = jax.random.normal(key_list[6], (GRID_H, RANK_H), jnp.float32) * GRID_H ** -0.5
    u_width = jax.random.normal(key_list[7], (GRID_W, RANK_W), jnp.float32) * GRID_W ** -0.5
    return {'tensor': tensor, 'u_time': u_time, 'u_height': u_height, 'u_width': u_width}


def operand_f32(matrix):
    return matrix.astype(jnp.bfloat16).astype(jnp.float32)


def col_normalise(power_cols):
    return power_cols / jnp.sqrt(jnp.sum(power_cols * power_cols, axis=0, keepdims=True))


def gram_update(unfold, factor):
    gram_mat = jnp.dot(unfold, unfold.T, preferred_element_type=jnp.float32).astype(jnp.bfloat16)
    return col_normalise(jnp.dot(gram_mat, factor.astype(jnp.bfloat16), preferred_element_type=jnp.float32))


def reference(tensor, u_time, u_height, u_width):
    t_full = jnp.dot(tensor.reshape(FRAMES * GRID_H, GRID_W), u_width.astype(jnp.bfloat16), preferred_element_type=jnp.float32)
    t_mat = t_full.astype(jnp.bfloat16).reshape(FRAMES, GRID_H, RANK_W).astype(jnp.float32)
    y_one = jnp.einsum('ihc,hb->ibc', t_mat, operand_f32(u_height)).astype(jnp.bfloat16)
    new_time = gram_update(y_one.reshape(FRAMES, RANK_H * RANK_W), u_time)
    y_two = jnp.einsum('ihc,ia->hac', t_mat, operand_f32(new_time)).astype(jnp.bfloat16)
    new_height = gram_update(y_two.reshape(GRID_H, RANK_T * RANK_W), u_height)
    z_flat = jnp.dot(new_time.astype(jnp.bfloat16).T, tensor.reshape(FRAMES, GRID_H * GRID_W), preferred_element_type=jnp.float32)
    z_mat = z_flat.astype(jnp.bfloat16).reshape(RANK_T, GRID_H, GRID_W).astype(jnp.float32)
    y_three = jnp.einsum('ahw,hb->wab', z_mat, operand_f32(new_height)).astype(jnp.bfloat16)
    new_width = gram_update(y_three.reshape(GRID_W, RANK_T * RANK_H), u_width)
    core_tensor = jnp.einsum('wab,wc->abc', y_three.astype(jnp.float32), operand_f32(new_width))
    core_energy = jnp.sum(core_tensor * core_tensor)
    return new_time, new_height, new_width, core_tensor, core_energy
```

```python
import functools

import jax
import jax.numpy as jnp
from jax import lax
from jax.experimental import pallas as pl
from jax.experimental.pallas import tpu as pltpu
from jax.sharding import PartitionSpec as P

MESH = pl.DeviceIdType.MESH
F32 = jnp.float32
BF16 = jnp.bfloat16
SIZE = {"z": 4, "y": 2, "x": 2, "c": 2}
ALL = ("z", "y", "x", "c")
LAG = 2
SLOTS = 4
ROWS = 96
STEP = 88


def place():
    a1 = lax.axis_index("a1")
    return {"z": lax.axis_index("a3"), "y": lax.axis_index("a2"), "x": a1 // 2, "c": lax.rem(a1, 2)}


def device(at):
    return (at["z"], at["y"], at["x"] * 2 + at["c"])


def member(at, group):
    index = 0
    for axis in group:
        index = index * SIZE[axis] + at[axis]
    return index


def moved(at, group, index):
    new = dict(at)
    for axis in reversed(group):
        new[axis] = lax.rem(index, SIZE[axis])
        index = index // SIZE[axis]
    return new


def total(group):
    count = 1
    for axis in group:
        count *= SIZE[axis]
    return count


def exchange(values, group, ident, gather=False):
    count = total(group)
    block = values.shape if gather else values.shape[1:]

    def kernel(src, dst, send, recv, own_sem):
        at = place()
        me = member(at, group)
        barrier = pltpu.get_barrier_semaphore()
        others = [lax.rem(me + step, count) for step in range(1, count)]
        for other in others:
            pl.semaphore_signal(barrier, inc=1, device_id=device(moved(at, group, other)), device_id_type=MESH)
        own = pltpu.make_async_copy(src if gather else src.at[me], dst.at[me], own_sem)
        own.start()
        pl.semaphore_wait(barrier, count - 1)
        copies = []
        for step, other in enumerate(others):
            copy = pltpu.make_async_remote_copy(
                src_ref=src if gather else src.at[other], dst_ref=dst.at[me],
                send_sem=send.at[step], recv_sem=recv.at[step],
                device_id=device(moved(at, group, other)), device_id_type=MESH)
            copy.start()
            copies.append(copy)
        own.wait()
        for copy in copies:
            copy.wait()

    return pl.pallas_call(
        kernel,
        out_shape=jax.ShapeDtypeStruct((count,) + tuple(block), values.dtype),
        in_specs=[pl.BlockSpec(memory_space=pltpu.VMEM)],
        out_specs=pl.BlockSpec(memory_space=pltpu.VMEM),
        scratch_shapes=[pltpu.SemaphoreType.DMA((count - 1,)), pltpu.SemaphoreType.DMA((count - 1,)), pltpu.SemaphoreType.DMA],
        compiler_params=pltpu.CompilerParams(collective_id=ident, has_side_effects=True, vmem_limit_bytes=48 * 1024 * 1024),
        name="exchange_" + "".join(group) + "_" + str(ident),
    )(values)


def width_kernel(x_hbm, u_ref, t_ref, x_all, x_vmem, s_up, r_up, s_dn, r_dn,
                 load_sem, ss_up, rs_up, ss_dn, rs_dn, free_up, free_dn, x_send, x_recv, own_sem):
    frames = x_hbm.shape[0]
    at = place()
    z = at["z"]
    me = at["x"] * 2 + at["c"]
    half = t_ref.shape[1]
    loads = []
    for part in range(frames // 8):
        rows = pl.ds(part * 8, 8)
        load = pltpu.make_async_copy(x_hbm.at[rows], x_vmem.at[rows], load_sem.at[part])
        load.start()
        loads.append(load)
    partners = []
    for flip in (1, 2, 3):
        new = dict(at)
        if flip & 1:
            new["c"] = 1 - at["c"]
        if flip & 2:
            new["x"] = 1 - at["x"]
        partners.append(new)
    barrier = pltpu.get_barrier_semaphore()
    for new in partners:
        pl.semaphore_signal(barrier, inc=1, device_id=device(new), device_id_type=MESH)

    @pl.when(z > 0)
    def _():
        pl.semaphore_signal(barrier, inc=1, device_id=device({**at, "z": z - 1}), device_id_type=MESH)

    @pl.when(z < 3)
    def _():
        pl.semaphore_signal(barrier, inc=1, device_id=device({**at, "z": z + 1}), device_id_type=MESH)

    pl.semaphore_wait(barrier, 3 + jnp.minimum(z, 1) + jnp.minimum(3 - z, 1))

    swaps = []
    for step, new in enumerate(partners):
        other = new["x"] * 2 + new["c"]
        swap = pltpu.make_async_remote_copy(
            src_ref=x_hbm.at[:, pl.ds(pl.multiple_of(other * STEP, 8), ROWS), :], dst_ref=x_all.at[me],
            send_sem=x_send.at[step], recv_sem=x_recv.at[step], device_id=device(new), device_id_type=MESH)
        swap.start()
        swaps.append(swap)

    @pl.when((z > 0) & (z < 3))
    def _():
        @pl.loop(0, frames)
        def _(frame):
            t_ref[frame] = jnp.zeros(t_ref.shape[1:], BF16)

    def stream(frame, first, last, toward, back, factor, sends, recvs, ss, rs, free):
        @pl.when((frame >= 0) & (frame < frames))
        def _():
            slot = lax.rem(frame, SLOTS)
            copy = pltpu.make_async_remote_copy(
                src_ref=sends.at[slot], dst_ref=recvs.at[slot], send_sem=ss.at[slot], recv_sem=rs.at[slot],
                device_id=device({**at, "z": toward}), device_id_type=MESH)
            part = lax.dot_general(factor, x_vmem[frame], (((1,), (1,)), ((), ())), preferred_element_type=F32)

            @pl.when((z != last) & (frame >= SLOTS))
            def _():
                copy.wait_send()
                pl.semaphore_wait(free, 1)

            sends[slot] = part

            @pl.when(z != first)
            def _():
                copy.wait_recv()
                sends[slot] += recvs[slot]

                @pl.when(frame + SLOTS < frames)
                def _():
                    pl.semaphore_signal(free, inc=1, device_id=device({**at, "z": back}), device_id_type=MESH)

            @pl.when(z != last)
            def _():
                copy.start()

            @pl.when(z == last)
            def _():
                t_ref[frame] = sends[slot].astype(BF16)

    above = jnp.minimum(z + 1, 3)
    below = jnp.maximum(z - 1, 0)
    lead = jnp.minimum(z, 3 - z)

    @pl.loop(0, frames + 3 * LAG)
    def _(step):
        newest = step - LAG * lead

        @pl.when((newest >= 0) & (newest < frames) & (lax.rem(newest, 8) == 0))
        def _():
            part = newest // 8
            rows = pl.ds(pl.multiple_of(part * 8, 8), 8)
            pltpu.make_async_copy(x_hbm.at[rows], x_vmem.at[rows], load_sem.at[part]).wait()

        stream(step - LAG * z, 0, 3, above, below, u_ref[half:], s_up, r_up, ss_up, rs_up, free_up)
        stream(step - LAG * (3 - z), 3, 0, below, above, u_ref[:half], s_dn, r_dn, ss_dn, rs_dn, free_dn)

    own = pltpu.make_async_copy(x_vmem.at[:, pl.ds(pl.multiple_of(me * STEP, 8), ROWS), :], x_all.at[me], own_sem)
    own.start()

    @pl.when(z < 3)
    def _():
        for slot in range(SLOTS):
            pltpu.make_async_remote_copy(
                src_ref=s_up.at[slot], dst_ref=r_up.at[slot], send_sem=ss_up.at[slot], recv_sem=rs_up.at[slot],
                device_id=device({**at, "z": above}), device_id_type=MESH).wait_send()

    @pl.when(z > 0)
    def _():
        for slot in range(SLOTS):
            pltpu.make_async_remote_copy(
                src_ref=s_dn.at[slot], dst_ref=r_dn.at[slot], send_sem=ss_dn.at[slot], recv_sem=rs_dn.at[slot],
                device_id=device({**at, "z": below}), device_id_type=MESH).wait_send()

    own.wait()
    for swap in swaps:
        swap.wait()


def width_product(tensor, factor_rows):
    frames, grid_h, grid_w = tensor.shape
    rank = factor_rows.shape[1]
    half = rank // 2
    link = pltpu.VMEM((SLOTS, half, grid_h), F32)
    any_space = pl.BlockSpec(memory_space=pl.ANY)
    vmem = pl.BlockSpec(memory_space=pltpu.VMEM)
    sems = pltpu.SemaphoreType.DMA
    return pl.pallas_call(
        width_kernel,
        out_shape=(jax.ShapeDtypeStruct((frames, half, grid_h), BF16),
                   jax.ShapeDtypeStruct((4, frames, ROWS, grid_w), BF16)),
        in_specs=[any_space, vmem],
        out_specs=(vmem, any_space),
        scratch_shapes=[pltpu.VMEM(tensor.shape, BF16), link, link, link, link,
                        sems((frames // 8,)), sems((SLOTS,)), sems((SLOTS,)), sems((SLOTS,)), sems((SLOTS,)),
                        pltpu.SemaphoreType.REGULAR, pltpu.SemaphoreType.REGULAR, sems((3,)), sems((3,)), sems],
        compiler_params=pltpu.CompilerParams(collective_id=1, has_side_effects=True, vmem_limit_bytes=60 * 1024 * 1024),
        name="width_product",
    )(tensor, factor_rows.T)


def time_kernel(u_ref, x_ref, z_ref, kron):
    @pl.when(pl.program_id(0) == 0)
    def _():
        shape = (u_ref.shape[1], kron.shape[1])
        picks = lax.broadcasted_iota(jnp.int32, shape, 1) // 8 == lax.broadcasted_iota(jnp.int32, shape, 0)
        spread = jnp.dot(u_ref[...], jnp.where(picks, 1.0, 0.0).astype(BF16), preferred_element_type=F32)
        same = lax.rem(lax.broadcasted_iota(jnp.int32, kron.shape, 0), 8) == lax.rem(lax.broadcasted_iota(jnp.int32, kron.shape, 1), 8)
        kron[...] = jnp.where(same, spread, 0.0).astype(BF16)

    for part in range(x_ref.shape[1] // 8):
        rows = slice(part * 8, part * 8 + 8)
        block = x_ref[:, rows, :]
        flat = block.reshape(block.shape[0] * 8, block.shape[2])
        out = jnp.dot(kron[...], flat, preferred_element_type=F32)
        z_ref[:, rows, :] = out.reshape(z_ref.shape[0], 8, out.shape[1]).astype(BF16)


def time_product(x_all, new_time):
    frames = x_all.shape[0] * x_all.shape[1]
    rows, grid_w = x_all.shape[2:]
    rank = new_time.shape[1]
    spread = jnp.repeat(new_time.astype(BF16).T, 8, axis=0)
    tile = 16
    return pl.pallas_call(
        time_kernel,
        grid=(rows // tile,),
        out_shape=jax.ShapeDtypeStruct((rank, rows, grid_w), BF16),
        in_specs=[pl.BlockSpec((rank * 8, frames), lambda i: (0, 0)),
                  pl.BlockSpec((frames, tile, grid_w), lambda i: (0, i, 0))],
        out_specs=pl.BlockSpec((rank, tile, grid_w), lambda i: (0, i, 0)),
        scratch_shapes=[pltpu.VMEM((rank * 8, frames * 8), BF16)],
        compiler_params=pltpu.CompilerParams(vmem_limit_bytes=60 * 1024 * 1024),
        name="time_product",
    )(spread, x_all.reshape(frames, rows, grid_w))


def height_kernel(u_ref, z_ref, y_ref):
    for a in range(z_ref.shape[1]):
        acc = None
        for s in range(z_ref.shape[0]):
            term = jnp.dot(u_ref[s], z_ref[s, a], preferred_element_type=F32)
            acc = term if acc is None else acc + term
        y_ref[a] = acc.astype(BF16)


def height_product(z_blocks, u_blocks):
    vmem = pl.BlockSpec(memory_space=pltpu.VMEM)
    return pl.pallas_call(
        height_kernel,
        out_shape=jax.ShapeDtypeStruct((z_blocks.shape[1], u_blocks.shape[1], z_blocks.shape[3]), BF16),
        in_specs=[vmem, vmem], out_specs=vmem,
        compiler_params=pltpu.CompilerParams(vmem_limit_bytes=48 * 1024 * 1024),
        name="height_product",
    )(u_blocks, z_blocks)


def normalise(power_cols):
    return power_cols / jnp.sqrt(jnp.sum(power_cols * power_cols, axis=0, keepdims=True))


def rows_of(factor, axis_name, count):
    return lax.dynamic_slice_in_dim(factor, lax.axis_index(axis_name) * count, count, 0).astype(BF16)


def solution(mesh):
    def local_sweep(tensor, u_time, u_height, u_width):
        frames, grid_h, grid_w = tensor.shape
        rank_t, rank_h, rank_w = u_time.shape[1], u_height.shape[1], u_width.shape[1]
        t_mat, x_all = width_product(tensor, rows_of(u_width, "a3", grid_w))

        y1_part = jnp.einsum("ich,hb->icb", t_mat, rows_of(u_height, "a2", grid_h), preferred_element_type=F32)
        y1_part = y1_part.reshape(frames, 2, -1).swapaxes(0, 1)
        y_one = exchange(y1_part, ("y",), 2).sum(0).astype(BF16)
        y_rows = exchange(y_one, ("x", "c"), 3, gather=True)
        gram = jnp.einsum("ik,rjk->irj", y_one, y_rows, preferred_element_type=F32).reshape(8, frames // 8, -1)
        gram = exchange(gram, ("z", "y"), 4).sum(0).astype(BF16)
        power = jnp.dot(gram, u_time.astype(BF16), preferred_element_type=F32)
        new_time = normalise(exchange(power, ("x", "c", "z", "y"), 5, gather=True).reshape(-1, rank_t))

        z_part = time_product(x_all, new_time)
        z_blocks = exchange(z_part.reshape(8, rank_t // 8, ROWS, grid_w), ("x", "c", "y"), 6)

        y2_part = jnp.einsum("ich,ia->ach", t_mat, rows_of(new_time, "a1", frames), preferred_element_type=F32)
        y2_part = y2_part.reshape(2, rank_t // 2, rank_w // 2, grid_h)
        y2_part = exchange(y2_part, ("c",), 7).sum(0).reshape(2, rank_t // 4, rank_w // 2, grid_h)
        y_two = exchange(y2_part, ("x",), 8).sum(0).astype(BF16).reshape(-1, grid_h)
        y_rows = exchange(y_two, ("y",), 9, gather=True)
        gram = jnp.einsum("kh,rkg->hrg", y_two, y_rows, preferred_element_type=F32).reshape(4, grid_h // 4, 2 * grid_h)
        gram = jnp.pad(gram, ((0, 0), (0, 6), (0, 0)))
        gram = exchange(gram, ("x", "c"), 10).sum(0).reshape(4, 24, 2 * grid_h)
        gram = exchange(gram, ("z",), 11).sum(0).astype(BF16)
        power = jnp.dot(gram, u_height.astype(BF16), preferred_element_type=F32)
        power = exchange(power, ("y", "x", "c", "z"), 12, gather=True)
        power = power.reshape(8, 96, rank_h)[:, :grid_h // 4].reshape(-1, rank_h)
        new_height = normalise(power)

        height_t = new_height.astype(BF16).T.reshape(rank_h, 2, grid_h)
        blocks = []
        for quarter in range(4):
            block = height_t[:, :, quarter * STEP:quarter * STEP + ROWS]
            if quarter < 3:
                block = jnp.where(jnp.arange(ROWS) < STEP, block, 0)
            blocks.append(block)
        u_blocks = jnp.stack(blocks).transpose(0, 2, 1, 3).reshape(8, rank_h, ROWS)
        y_three = height_product(z_blocks, u_blocks)
        y_flat = y_three.reshape(-1, grid_w)
        y_rows = exchange(y_flat, ("z",), 13, gather=True)
        gram = jnp.einsum("kw,rkv->wrv", y_flat, y_rows, preferred_element_type=F32).reshape(8, grid_w // 8, 4 * grid_w)
        gram = exchange(gram, ("y", "x", "c"), 14).sum(0).astype(BF16)
        power = jnp.dot(gram, u_width.astype(BF16), preferred_element_type=F32)
        power = exchange(power.reshape(-1, 128), ALL, 15, gather=True)
        new_width = normalise(power.reshape(-1, rank_w))

        core = jnp.dot(y_flat, rows_of(new_width, "a3", grid_w), preferred_element_type=F32)
        core = core.reshape(rank_t // 8, 2, rank_h // 2, 4, rank_w // 4).transpose(3, 1, 0, 2, 4)
        core = exchange(core.reshape(8, rank_t // 8, -1), ("z", "y"), 16)
        core = core.reshape(4, rank_t // 4, -1).sum(0)
        core_tensor = core.reshape(rank_t // 4, rank_h // 2, rank_w // 4)
        energy = jnp.full((8, 128), jnp.sum(core_tensor * core_tensor))
        core_energy = jnp.sum(exchange(energy, ALL, 17, gather=True)[:, 0, 0])
        return new_time, new_height, new_width, core_tensor, core_energy

    return jax.shard_map(local_sweep, mesh=mesh, in_specs=(P("a1", "a2", "a3"), P(), P(), P()), out_specs=(P(), P(), P(), P("a1", "a2", "a3"), P()), check_vma=False)
```

```python
import functools

import jax
import jax.numpy as jnp
from jax import lax
from jax.experimental import pallas as pl
from jax.experimental.pallas import tpu as pltpu
from jax.sharding import PartitionSpec as P

MESH = pl.DeviceIdType.MESH
F32 = jnp.float32
BF16 = jnp.bfloat16
SIZE = {"z": 4, "y": 2, "x": 2, "c": 2}
ALL = ("z", "y", "x", "c")
LAG = 2
SLOTS = 4


def place():
    a1 = lax.axis_index("a1")
    return {"z": lax.axis_index("a3"), "y": lax.axis_index("a2"), "x": a1 // 2, "c": lax.rem(a1, 2)}


def device(at):
    return (at["z"], at["y"], at["x"] * 2 + at["c"])


def member(at, group):
    index = 0
    for axis in group:
        index = index * SIZE[axis] + at[axis]
    return index


def moved(at, group, index):
    new = dict(at)
    for axis in reversed(group):
        new[axis] = lax.rem(index, SIZE[axis])
        index = index // SIZE[axis]
    return new


def total(group):
    count = 1
    for axis in group:
        count *= SIZE[axis]
    return count


def exchange(values, group, ident, gather=False):
    count = total(group)
    block = values.shape if gather else values.shape[1:]

    def kernel(src, dst, send, recv, own_sem):
        at = place()
        me = member(at, group)
        barrier = pltpu.get_barrier_semaphore()
        others = [lax.rem(me + step, count) for step in range(1, count)]
        for other in others:
            pl.semaphore_signal(barrier, inc=1, device_id=device(moved(at, group, other)), device_id_type=MESH)
        own = pltpu.make_async_copy(src if gather else src.at[me], dst.at[me], own_sem)
        own.start()
        pl.semaphore_wait(barrier, count - 1)
        copies = []
        for step, other in enumerate(others):
            copy = pltpu.make_async_remote_copy(
                src_ref=src if gather else src.at[other], dst_ref=dst.at[me],
                send_sem=send.at[step], recv_sem=recv.at[step],
                device_id=device(moved(at, group, other)), device_id_type=MESH)
            copy.start()
            copies.append(copy)
        own.wait()
        for copy in copies:
            copy.wait()

    return pl.pallas_call(
        kernel,
        out_shape=jax.ShapeDtypeStruct((count,) + tuple(block), values.dtype),
        in_specs=[pl.BlockSpec(memory_space=pltpu.VMEM)],
        out_specs=pl.BlockSpec(memory_space=pltpu.VMEM),
        scratch_shapes=[pltpu.SemaphoreType.DMA((count - 1,)), pltpu.SemaphoreType.DMA((count - 1,)), pltpu.SemaphoreType.DMA],
        compiler_params=pltpu.CompilerParams(collective_id=ident, has_side_effects=True, vmem_limit_bytes=48 * 1024 * 1024),
        name="exchange_" + "".join(group) + "_" + str(ident),
    )(values)


BATCH = 16


def edge_member(at):
    return ((at["x"] * 2 + at["c"]) * 2 + at["z"] // 3) * 2 + at["y"]


def first_kernel(x_hbm, u3_ref, u2_ref, u1_ref, t_ref, x_all, new_ref, x_vmem, s_up, r_up, s_dn, r_dn,
                 y_part, y_recv, y_all, g_part, g_recv, p_send, p_all,
                 load_sem, ss_up, rs_up, ss_dn, rs_dn, free_up, free_dn, x_send, x_recv, own_sem,
                 y_ss, y_rs, c_ss, c_rs, w_ss, w_rs, f_ss, f_rs, g_ss, g_rs, p_ss, p_rs):
    frames = x_hbm.shape[0]
    at = place()
    z = at["z"]
    me = at["x"] * 2 + at["c"]
    half = t_ref.shape[1]
    quarter = x_all.shape[2]
    mine = member(at, ALL)
    edge = (z == 0) | (z == 3)
    loads = frames // 8
    for part in range(loads):
        rows = pl.ds(part * 8, 8)
        pltpu.make_async_copy(x_hbm.at[rows], x_vmem.at[rows], load_sem.at[part]).start()
    barrier = pltpu.get_barrier_semaphore()
    for step in range(1, 32):
        other = moved(at, ALL, lax.rem(mine + step, 32))
        pl.semaphore_signal(barrier, inc=1, device_id=device(other), device_id_type=MESH)
    pl.semaphore_wait(barrier, 31)

    core_pair = {**at, "c": 1 - at["c"]}
    x_pair = {**at, "x": 1 - at["x"]}
    y_pair = {**at, "y": 1 - at["y"]}
    partners = [core_pair, x_pair, {**core_pair, "x": 1 - at["x"]}]
    swaps = []
    for step, new in enumerate(partners):
        other = new["x"] * 2 + new["c"]
        swap = pltpu.make_async_remote_copy(
            src_ref=x_hbm.at[:, pl.ds(pl.multiple_of(other * quarter, 16), quarter), :], dst_ref=x_all.at[me],
            send_sem=x_send.at[step], recv_sem=x_recv.at[step], device_id=device(new), device_id_type=MESH)
        swap.start()
        swaps.append(swap)

    @pl.when(jnp.logical_not(edge))
    def _():
        @pl.loop(0, frames)
        def _(frame):
            t_ref[frame] = jnp.zeros(t_ref.shape[1:], BF16)

    def stream(frame, first, last, toward, back, factor, sends, recvs, ss, rs, free):
        @pl.when((frame >= 0) & (frame < frames))
        def _():
            slot = lax.rem(frame, SLOTS)
            copy = pltpu.make_async_remote_copy(
                src_ref=sends.at[slot], dst_ref=recvs.at[slot], send_sem=ss.at[slot], recv_sem=rs.at[slot],
                device_id=device({**at, "z": toward}), device_id_type=MESH)
            part = jnp.dot(factor, x_vmem[frame], preferred_element_type=F32)

            @pl.when((z != last) & (frame >= SLOTS))
            def _():
                copy.wait_send()
                pl.semaphore_wait(free, 1)

            sends[slot] = part

            @pl.when(z != first)
            def _():
                copy.wait_recv()
                sends[slot] += recvs[slot]

                @pl.when(frame + SLOTS < frames)
                def _():
                    pl.semaphore_signal(free, inc=1, device_id=device({**at, "z": back}), device_id_type=MESH)

            @pl.when(z != last)
            def _():
                copy.start()

            @pl.when(z == last)
            def _():
                done = sends[slot].astype(BF16)
                t_ref[frame] = done
                rows = jnp.dot(done, u2_ref[...], preferred_element_type=F32)
                y_part[:, pl.ds(frame, 1), :] = rows[:, None, :]

    keep = pl.ds(at["y"] * (half // 2), half // 2)
    give = pl.ds((1 - at["y"]) * (half // 2), half // 2)

    def rows_at(batch):
        return pl.ds(pl.multiple_of(batch * BATCH, BATCH), BATCH)

    def y_copy(batch):
        return pltpu.make_async_remote_copy(
            src_ref=y_part.at[give, rows_at(batch), :], dst_ref=y_recv.at[:, rows_at(batch), :],
            send_sem=y_ss.at[batch], recv_sem=y_rs.at[batch], device_id=device(y_pair), device_id_type=MESH)

    def spread_copy(owner, batch, pair, ss, rs):
        block = y_all.at[owner, :, rows_at(batch), :]
        return pltpu.make_async_remote_copy(
            src_ref=block, dst_ref=block, send_sem=ss.at[batch], recv_sem=rs.at[batch],
            device_id=device(pair), device_id_type=MESH)

    far = x_pair["x"] * 2 + at["c"]

    def settle(batch):
        y_copy(batch).wait_recv()
        rows = rows_at(batch)
        y_all[me, :, rows, :] = (y_part[keep, rows, :] + y_recv[:, rows, :]).astype(BF16)
        spread_copy(me, batch, core_pair, c_ss, c_rs).start()
        spread_copy(me, batch, x_pair, w_ss, w_rs).start()

    def forward(batch):
        spread_copy(me, batch, x_pair, w_ss, w_rs).wait_recv()
        spread_copy(far, batch, core_pair, f_ss, f_rs).start()

    above = jnp.minimum(z + 1, 3)
    below = jnp.maximum(z - 1, 0)
    lead = jnp.minimum(z, 3 - z)

    @pl.loop(0, frames + 3 * LAG)
    def _(step):
        newest = step - LAG * lead

        @pl.when((newest >= 0) & (newest < frames) & (lax.rem(newest, 8) == 0))
        def _():
            part = newest // 8
            rows = pl.ds(pl.multiple_of(part * 8, 8), 8)
            pltpu.make_async_copy(x_hbm.at[rows], x_vmem.at[rows], load_sem.at[part]).wait()

        stream(step - LAG * z, 0, 3, above, below, u3_ref[half:], s_up, r_up, ss_up, rs_up, free_up)
        stream(step - LAG * (3 - z), 3, 0, below, above, u3_ref[:half], s_dn, r_dn, ss_dn, rs_dn, free_dn)
        final = step - 3 * LAG

        @pl.when(edge & (final >= 0))
        def _():
            place_in = lax.rem(final, BATCH)
            batch = final // BATCH

            @pl.when(place_in == BATCH - 1)
            def _():
                y_copy(batch).start()

            @pl.when((place_in == BATCH // 2) & (batch >= 1))
            def _():
                settle(batch - 1)

            @pl.when((place_in == BATCH // 2) & (batch >= 2))
            def _():
                forward(batch - 2)

    own = pltpu.make_async_copy(x_vmem.at[:, pl.ds(pl.multiple_of(me * quarter, 16), quarter), :], x_all.at[me], own_sem)
    own.start()
    batches = frames // BATCH
    last_batch = batches - 1

    j = (z // 3) * 2 + at["y"]
    piece = frames // 4
    quads = []
    for flip in (1, 2, 3):
        new = dict(at)
        if flip & 1:
            new["y"] = 1 - at["y"]
        if flip & 2:
            new["z"] = 3 - z
        quads.append(new)

    def g_copy(step, new):
        to = (new["z"] // 3) * 2 + new["y"]
        return pltpu.make_async_remote_copy(
            src_ref=g_part.at[:, pl.ds(pl.multiple_of(to * piece, 8), piece), :], dst_ref=g_recv.at[step],
            send_sem=g_ss.at[step], recv_sem=g_rs.at[step], device_id=device(new), device_id_type=MESH)

    slot16 = edge_member(at)

    def p_copy(step):
        other = moved(at, ALL, lax.rem(mine + step, 32))
        return pltpu.make_async_remote_copy(
            src_ref=p_send, dst_ref=p_all.at[slot16], send_sem=p_ss.at[step - 1], recv_sem=p_rs.at[slot16],
            device_id=device(other), device_id_type=MESH)

    @pl.when(edge)
    def _():
        settle(last_batch)
        forward(last_batch - 1)
        forward(last_batch)
        for batch in range(batches):
            spread_copy(me, batch, core_pair, c_ss, c_rs).wait_recv()
            spread_copy(far, batch, core_pair, f_ss, f_rs).wait_recv()
        g_part[...] = jnp.zeros(g_part.shape, F32)

        @pl.loop(0, half // 2)
        def _(col):
            left = y_all[me, col]
            for r in range(4):
                g_part[r] += lax.dot_general(left, y_all[r, col], (((1,), (1,)), ((), ())), preferred_element_type=F32)

        for step, new in enumerate(quads):
            g_copy(step, new).start()
        rows = pl.ds(pl.multiple_of(j * piece, 8), piece)
        for step, new in enumerate(quads):
            g_copy(step, new).wait_recv()
        power = None
        for r in range(4):
            gram = g_part[r, rows, :] + g_recv[0, r] + g_recv[1, r] + g_recv[2, r]
            term = jnp.dot(gram.astype(BF16), u1_ref[r], preferred_element_type=F32)
            power = term if power is None else power + term
        p_send[...] = power
        p_all[slot16] = power
        for step in range(1, 32):
            p_copy(step).start()
        for step, new in enumerate(quads):
            g_copy(step, new).wait_send()
        for batch in range(batches):
            y_copy(batch).wait_send()
            spread_copy(me, batch, core_pair, c_ss, c_rs).wait_send()
            spread_copy(me, batch, x_pair, w_ss, w_rs).wait_send()
            spread_copy(far, batch, core_pair, f_ss, f_rs).wait_send()

    for source in range(16):
        @pl.when(jnp.logical_not(edge) | (slot16 != source))
        def _():
            pltpu.make_async_remote_copy(
                src_ref=p_send, dst_ref=p_all.at[source], send_sem=p_ss.at[0], recv_sem=p_rs.at[source],
                device_id=device(moved(at, ALL, lax.rem(mine + 1, 32))), device_id_type=MESH).wait_recv()

    squares = jnp.sum(jnp.sum(p_all[...] * p_all[...], axis=0), axis=0, keepdims=True)
    new_ref[...] = p_all[...] / jnp.sqrt(squares)[None]

    @pl.when(edge)
    def _():
        for step in range(1, 32):
            p_copy(step).wait_send()

    @pl.when(z < 3)
    def _():
        for slot in range(SLOTS):
            pltpu.make_async_remote_copy(
                src_ref=s_up.at[slot], dst_ref=r_up.at[slot], send_sem=ss_up.at[slot], recv_sem=rs_up.at[slot],
                device_id=device({**at, "z": above}), device_id_type=MESH).wait_send()

    @pl.when(z > 0)
    def _():
        for slot in range(SLOTS):
            pltpu.make_async_remote_copy(
                src_ref=s_dn.at[slot], dst_ref=r_dn.at[slot], send_sem=ss_dn.at[slot], recv_sem=rs_dn.at[slot],
                device_id=device({**at, "z": below}), device_id_type=MESH).wait_send()

    own.wait()
    for swap in swaps:
        swap.wait()


def first_stage(tensor_t, u3_rows, u2_rows, u1):
    frames, grid_w, grid_h = tensor_t.shape
    half, rank_h, rank_t = u3_rows.shape[1] // 2, u2_rows.shape[1], u1.shape[1]
    link = pltpu.VMEM((SLOTS, half, grid_h), F32)
    any_space = pl.BlockSpec(memory_space=pl.ANY)
    vmem = pl.BlockSpec(memory_space=pltpu.VMEM)
    sems = pltpu.SemaphoreType.DMA
    regular = pltpu.SemaphoreType.REGULAR
    batches = frames // BATCH
    piece = frames // 4
    return pl.pallas_call(
        first_kernel,
        out_shape=(jax.ShapeDtypeStruct((frames, half, grid_h), BF16),
                   jax.ShapeDtypeStruct((4, frames, grid_w // 4, grid_h), BF16),
                   jax.ShapeDtypeStruct((16, piece, rank_t), F32)),
        in_specs=[any_space, vmem, vmem, vmem],
        out_specs=(vmem, any_space, vmem),
        scratch_shapes=[pltpu.VMEM(tensor_t.shape, BF16), link, link, link, link,
                        pltpu.VMEM((half, frames, rank_h), F32), pltpu.VMEM((half // 2, frames, rank_h), F32),
                        pltpu.VMEM((4, half // 2, frames, rank_h), BF16),
                        pltpu.VMEM((4, frames, frames), F32), pltpu.VMEM((3, 4, piece, frames), F32),
                        pltpu.VMEM((piece, rank_t), F32), pltpu.VMEM((16, piece, rank_t), F32),
                        sems((frames // 8,)), sems((SLOTS,)), sems((SLOTS,)), sems((SLOTS,)), sems((SLOTS,)),
                        regular, regular, sems((3,)), sems((3,)), sems,
                        sems((batches,)), sems((batches,)), sems((batches,)), sems((batches,)),
                        sems((batches,)), sems((batches,)), sems((batches,)), sems((batches,)),
                        sems((3,)), sems((3,)), sems((31,)), sems((16,))],
        compiler_params=pltpu.CompilerParams(collective_id=1, has_side_effects=True, vmem_limit_bytes=60 * 1024 * 1024),
        name="first_stage",
    )(tensor_t, u3_rows.T, u2_rows, u1.astype(BF16).reshape(4, frames, rank_t))


def time_kernel(u_ref, x_ref, z_ref, kron):
    @pl.when(pl.program_id(0) == 0)
    def _():
        shape = (u_ref.shape[1], kron.shape[1])
        picks = lax.broadcasted_iota(jnp.int32, shape, 1) // 8 == lax.broadcasted_iota(jnp.int32, shape, 0)
        spread = jnp.dot(u_ref[...], jnp.where(picks, 1.0, 0.0).astype(BF16), preferred_element_type=F32)
        same = lax.rem(lax.broadcasted_iota(jnp.int32, kron.shape, 0), 8) == lax.rem(lax.broadcasted_iota(jnp.int32, kron.shape, 1), 8)
        kron[...] = jnp.where(same, spread, 0.0).astype(BF16)

    for part in range(x_ref.shape[1] // 8):
        rows = slice(part * 8, part * 8 + 8)
        block = x_ref[:, rows, :]
        flat = block.reshape(block.shape[0] * 8, block.shape[2])
        out = jnp.dot(kron[...], flat, preferred_element_type=F32)
        z_ref[:, rows, :] = out.reshape(z_ref.shape[0], 8, out.shape[1]).astype(BF16)


def time_product(x_all, new_time):
    frames = x_all.shape[0] * x_all.shape[1]
    rows, grid_w = x_all.shape[2:]
    rank = new_time.shape[1]
    spread = jnp.repeat(new_time.astype(BF16).T, 8, axis=0)
    tile = 16
    return pl.pallas_call(
        time_kernel,
        grid=(rows // tile,),
        out_shape=jax.ShapeDtypeStruct((rank, rows, grid_w), BF16),
        in_specs=[pl.BlockSpec((rank * 8, frames), lambda i: (0, 0)),
                  pl.BlockSpec((frames, tile, grid_w), lambda i: (0, i, 0))],
        out_specs=pl.BlockSpec((rank, tile, grid_w), lambda i: (0, i, 0)),
        scratch_shapes=[pltpu.VMEM((rank * 8, frames * 8), BF16)],
        compiler_params=pltpu.CompilerParams(vmem_limit_bytes=60 * 1024 * 1024),
        name="time_product",
    )(spread, x_all.reshape(frames, rows, grid_w))


def height_kernel(u_ref, z_ref, y_ref):
    for group in range(y_ref.shape[0]):
        block = None
        for s in range(z_ref.shape[0]):
            flat = z_ref[s, group].reshape(-1, z_ref.shape[-1])
            term = jnp.dot(flat, u_ref[s], preferred_element_type=F32)
            block = term if block is None else block + term
        y_ref[group] = block.astype(BF16)


def height_product(z_blocks, u_blocks):
    vmem = pl.BlockSpec(memory_space=pltpu.VMEM)
    _, groups, many, width, _ = z_blocks.shape
    return pl.pallas_call(
        height_kernel,
        out_shape=jax.ShapeDtypeStruct((groups, many * width, u_blocks.shape[2]), BF16),
        in_specs=[vmem, vmem], out_specs=vmem,
        compiler_params=pltpu.CompilerParams(vmem_limit_bytes=48 * 1024 * 1024),
        name="height_product",
    )(u_blocks, z_blocks)


def normalise(power_cols):
    return power_cols / jnp.sqrt(jnp.sum(power_cols * power_cols, axis=0, keepdims=True))


def rows_of(factor, axis_name, count):
    return lax.dynamic_slice_in_dim(factor, lax.axis_index(axis_name) * count, count, 0).astype(BF16)


def solution(mesh):
    def local_sweep(tensor, u_time, u_height, u_width):
        frames, grid_h, grid_w = tensor.shape
        rank_t, rank_h, rank_w = u_time.shape[1], u_height.shape[1], u_width.shape[1]
        t_mat, x_all, new_time = first_stage(tensor.swapaxes(1, 2), rows_of(u_width, "a3", grid_w), rows_of(u_height, "a2", grid_h), u_time)
        new_time = new_time.reshape(-1, rank_t)

        ordered = new_time.reshape(-1, 4, 2, rank_t // 8).swapaxes(1, 2).reshape(-1, rank_t)
        z_part = time_product(x_all, ordered)
        z_blocks = exchange(z_part.reshape(2, rank_t // 2, grid_w // 4, grid_h), ("y",), 6)

        y2_part = jnp.einsum("ich,ia->ach", t_mat, rows_of(new_time, "a1", frames), preferred_element_type=F32)
        y2_part = y2_part.reshape(2, rank_t // 2, rank_w // 2, grid_h)
        y2_part = exchange(y2_part, ("c",), 7).sum(0).reshape(2, rank_t // 4, rank_w // 2, grid_h)
        y_two = exchange(y2_part, ("x",), 8).sum(0).astype(BF16).reshape(-1, grid_h)
        y_rows = exchange(y_two, ("y",), 9, gather=True)
        gram = jnp.einsum("kh,rkg->hrg", y_two, y_rows, preferred_element_type=F32).reshape(4, grid_h // 4, 2 * grid_h)
        gram = jnp.pad(gram, ((0, 0), (0, 6), (0, 0)))
        gram = exchange(gram, ("x", "c"), 10).sum(0).reshape(4, 24, 2 * grid_h)
        gram = exchange(gram, ("z",), 11).sum(0).astype(BF16)
        power = jnp.dot(gram, u_height.astype(BF16), preferred_element_type=F32)
        power = exchange(power, ("y", "x", "c", "z"), 12, gather=True)
        power = power.reshape(8, 96, rank_h)[:, :grid_h // 4].reshape(-1, rank_h)
        new_height = normalise(power)

        u_blocks = new_height.astype(BF16).reshape(2, grid_h, rank_h)
        y_three = height_product(z_blocks.reshape(2, 4, rank_t // 8, grid_w // 4, grid_h), u_blocks)
        y_three = exchange(y_three, ("x", "c"), 2).reshape(4, rank_t // 8, grid_w // 4, rank_h)
        y_flat = y_three.transpose(1, 3, 0, 2).reshape(-1, grid_w)
        y_rows = exchange(y_flat, ("z",), 13, gather=True)
        gram = jnp.einsum("kw,rkv->wrv", y_flat, y_rows, preferred_element_type=F32).reshape(8, grid_w // 8, 4 * grid_w)
        gram = exchange(gram, ("y", "x", "c"), 14).sum(0).astype(BF16)
        power = jnp.dot(gram, u_width.astype(BF16), preferred_element_type=F32)
        power = exchange(power.reshape(-1, 128), ALL, 15, gather=True)
        new_width = normalise(power.reshape(-1, rank_w))

        core = jnp.dot(y_flat, rows_of(new_width, "a3", grid_w), preferred_element_type=F32)
        core = core.reshape(rank_t // 8, 2, rank_h // 2, 4, rank_w // 4).transpose(3, 1, 0, 2, 4)
        core = exchange(core.reshape(8, rank_t // 8, -1), ("z", "y"), 16)
        core = core.reshape(4, rank_t // 4, -1).sum(0)
        core_tensor = core.reshape(rank_t // 4, rank_h // 2, rank_w // 4)
        energy = jnp.full((8, 128), jnp.sum(core_tensor * core_tensor))
        core_energy = jnp.sum(exchange(energy, ALL, 17, gather=True)[:, 0, 0])
        return new_time, new_height, new_width, core_tensor, core_energy

    return jax.shard_map(local_sweep, mesh=mesh, in_specs=(P("a1", "a2", "a3"), P(), P(), P()), out_specs=(P(), P(), P(), P("a1", "a2", "a3"), P()), check_vma=False)
```

```python
import jax
import jax.numpy as jnp
from jax import lax
from jax.experimental import pallas as pl
from jax.experimental.pallas import tpu as pltpu
from jax.sharding import PartitionSpec as P

MESH = pl.DeviceIdType.MESH
F32 = jnp.float32
BF16 = jnp.bfloat16
SIZE = {"z": 4, "y": 2, "x": 2, "c": 2}
ALL = ("z", "y", "x", "c")
COUNT = 32
OTHERS = range(1, COUNT)
PLANE = ("c", "x", "y", "xc", "yc", "yx", "yxc")
LAG = 2
SLOTS = 8
BATCH = 16
TILE = 8
PAD = 48
EDGE = 3
NT = (((1,), (1,)), ((), ()))
TN = (((0,), (0,)), ((), ()))
LIMIT = 60 * 1024 * 1024


def place():
    a1 = lax.axis_index("a1")
    return {"z": lax.axis_index("a3"), "y": lax.axis_index("a2"), "x": a1 // 2, "c": lax.rem(a1, 2)}


def device(at):
    return (at["z"], at["y"], at["x"] * 2 + at["c"])


def block_of(at):
    return at["x"] * 2 + at["c"]


def member(at, group):
    index = 0
    for axis in group:
        index = index * SIZE[axis] + at[axis]
    return index


def flip(at, axes):
    return {axis: SIZE[axis] - 1 - at[axis] if axis in axes else at[axis] for axis in at}


def ahead(at, step):
    index = lax.rem(member(at, ALL) + step, COUNT)
    new = {}
    for axis in reversed(ALL):
        new[axis] = lax.rem(index, SIZE[axis])
        index = index // SIZE[axis]
    return new


def remote(src, dst, ss, rs, to):
    return pltpu.make_async_remote_copy(src_ref=src, dst_ref=dst, send_sem=ss, recv_sem=rs, device_id=device(to), device_id_type=MESH)


def greet(at):
    barrier = pltpu.get_barrier_semaphore()
    for step in OTHERS:
        pl.semaphore_signal(barrier, inc=1, device_id=device(ahead(at, step)), device_id_type=MESH)
    return barrier


def aligned(start, size):
    return pl.ds(pl.multiple_of(start, TILE), size)


def column_norm(power, axes):
    return jnp.sqrt(jnp.sum(power * power, axis=axes, keepdims=True))


def eights(shape, axis):
    return lax.broadcasted_iota(jnp.int32, shape, axis) // TILE


def in_eight(shape, axis):
    return lax.rem(lax.broadcasted_iota(jnp.int32, shape, axis), TILE)


def spread_blocks(rank, values, at, kron):
    blocks, _, width = kron.shape
    shape = (rank * TILE, rank)
    row = eights(shape, 0)
    sixth = rank // TILE
    quarter = row // sixth
    wanted = (lax.rem(quarter, 4) * 2 + quarter // 4) * sixth + lax.rem(row, sixth)
    picks = jnp.where(lax.broadcasted_iota(jnp.int32, shape, 1) == wanted, 1.0, 0.0).astype(BF16)
    spread = lax.dot_general(picks, values, NT, preferred_element_type=F32).astype(BF16)
    for block in range(blocks):
        shape = (values.shape[0], width)
        match = eights(shape, 1) + block * (width // TILE) == lax.broadcasted_iota(jnp.int32, shape, 0)
        wide = jnp.dot(spread, jnp.where(match, 1.0, 0.0).astype(BF16), preferred_element_type=F32)
        same = in_eight(wide.shape, 0) == in_eight(wide.shape, 1)
        kron[block] = jnp.where(same, wide, 0.0).astype(BF16)


def first_kernel(x_hbm, x_tiles, u3_ref, u2_ref, u1_ref, t_ref, x_all, new_ref, x_vmem, u3_rows, u2_rows, u1_rows, s_up, r_up, s_dn, r_dn,
                 own_tiles, y_part, y_recv, y_all, g_part, g_recv, p_send, p_all, free_up, free_dn, own_in, own_sem,
                 load_sem, ss_up, rs_up, ss_dn, rs_dn, x_send, x_recv,
                 y_ss, y_rs, c_ss, c_rs, w_ss, w_rs, f_ss, f_rs, g_ss, g_rs, p_ss, p_rs):
    frames, grid_w, grid_h = x_hbm.shape
    at = place()
    z, y = at["z"], at["y"]
    me = block_of(at)
    half = t_ref.shape[0] * TILE
    groups = x_all.shape[2]
    last = SIZE["z"] - 1
    edge = (z == 0) | (z == last)
    for part in range(frames // TILE):
        rows = pl.ds(part * TILE, TILE)
        pltpu.make_async_copy(x_hbm.at[rows], x_vmem.at[rows], load_sem.at[part]).start()
    barrier = greet(at)
    own = pltpu.make_async_copy(x_tiles.at[:, pl.ds(me * groups, groups)], own_tiles, own_in)
    own.start()
    for index in range(SIZE["z"]):
        @pl.when(z == index)
        def _():
            u3_rows[...] = u3_ref[:, index * grid_w:(index + 1) * grid_w].astype(BF16)

    for index in range(SIZE["y"]):
        @pl.when(y == index)
        def _():
            u2_rows[...] = u2_ref[:, index * grid_h:(index + 1) * grid_h].astype(BF16)

    for index in range(u1_rows.shape[0]):
        u1_rows[index] = u1_ref[:, index * frames:(index + 1) * frames].astype(BF16)

    @pl.when(jnp.logical_not(edge))
    def _():
        @pl.loop(0, frames)
        def _(frame):
            t_ref[:, frame] = jnp.zeros((half // TILE, TILE, grid_h), BF16)

    pl.semaphore_wait(barrier, COUNT - 1)

    core_pair, x_pair, y_pair = flip(at, "c"), flip(at, "x"), flip(at, "y")
    partners = [core_pair, x_pair, flip(at, "xc")]

    def swap_copy(way, frame):
        new = partners[way]
        return remote(x_tiles.at[frame, pl.ds(block_of(new) * groups, groups)], x_all.at[me, frame], x_send.at[way], x_recv.at[way], new)

    def link(slot, up):
        if up:
            return remote(s_up.at[slot], r_up.at[slot], ss_up.at[slot], rs_up.at[slot], {**at, "z": above})
        return remote(s_dn.at[slot], r_dn.at[slot], ss_dn.at[slot], rs_dn.at[slot], {**at, "z": below})

    def stream(frame, up):
        start, end, back, factor = (0, last, below, u3_rows[half:]) if up else (last, 0, above, u3_rows[:half])
        sends, recvs, free = (s_up, r_up, free_up) if up else (s_dn, r_dn, free_dn)

        @pl.when((frame >= 0) & (frame < frames))
        def _():
            slot = lax.rem(frame, SLOTS)
            copy = link(slot, up)
            part = jnp.dot(factor, x_vmem[frame], preferred_element_type=F32)

            @pl.when((z != end) & (frame >= SLOTS))
            def _():
                copy.wait_send()
                pl.semaphore_wait(free, 1)

            sends[slot] = part

            @pl.when(z != start)
            def _():
                copy.wait_recv()
                sends[slot] += recvs[slot]

                @pl.when(frame + SLOTS < frames)
                def _():
                    pl.semaphore_signal(free, inc=1, device_id=device({**at, "z": back}), device_id_type=MESH)

            @pl.when(z != end)
            def _():
                copy.start()

            @pl.when(z == end)
            def _():
                done = sends[slot].astype(BF16)
                t_ref[:, frame] = done.reshape(half // TILE, TILE, grid_h)
                rows = lax.dot_general(done, u2_rows[...], NT, preferred_element_type=F32)
                y_part[:, pl.ds(frame, 1), :] = rows[:, None, :]

    side = half // 2
    keep, give = pl.ds(y * side, side), pl.ds((1 - y) * side, side)

    def rows_at(batch):
        return pl.ds(pl.multiple_of(batch * BATCH, BATCH), BATCH)

    def y_copy(batch):
        rows = rows_at(batch)
        return remote(y_part.at[give, rows, :], y_recv.at[:, rows, :], y_ss.at[batch], y_rs.at[batch], y_pair)

    def spread_copy(owner, batch, pair, ss, rs):
        block = y_all.at[owner, :, rows_at(batch), :]
        return remote(block, block, ss.at[batch], rs.at[batch], pair)

    far = block_of(x_pair)

    def settle(batch):
        y_copy(batch).wait_recv()
        rows = rows_at(batch)
        y_all[me, :, rows, :] = (y_part[keep, rows, :] + y_recv[:, rows, :]).astype(BF16)
        spread_copy(me, batch, core_pair, c_ss, c_rs).start()
        spread_copy(me, batch, x_pair, w_ss, w_rs).start()

    def forward(batch):
        spread_copy(me, batch, x_pair, w_ss, w_rs).wait_recv()
        spread_copy(far, batch, core_pair, f_ss, f_rs).start()

    own.wait()
    put = pltpu.make_async_copy(own_tiles, x_all.at[me], own_sem)
    put.start()
    above = jnp.minimum(z + 1, last)
    below = jnp.maximum(z - 1, 0)
    lead = jnp.minimum(z, last - z)

    @pl.loop(0, frames + last * LAG)
    def _(step):
        newest = step - LAG * lead

        @pl.when(step < frames)
        def _():
            for way in range(len(partners)):
                swap_copy(way, jnp.minimum(step, frames - 1)).start()

        @pl.when((newest >= 0) & (newest < frames) & (lax.rem(newest, TILE) == 0))
        def _():
            part = newest // TILE
            rows = aligned(part * TILE, TILE)
            pltpu.make_async_copy(x_hbm.at[rows], x_vmem.at[rows], load_sem.at[part]).wait()

        stream(step - LAG * z, True)
        stream(step - LAG * (last - z), False)
        final = step - last * LAG

        @pl.when(edge & (final >= 0))
        def _():
            place_in = lax.rem(final, BATCH)
            batch = final // BATCH

            @pl.when(place_in == BATCH - 1)
            def _():
                y_copy(batch).start()

            @pl.when((place_in == BATCH // 2) & (batch >= 1))
            def _():
                settle(batch - 1)

            @pl.when((place_in == BATCH // 2) & (batch >= 3))
            def _():
                forward(batch - 3)

    batches = frames // BATCH
    piece = frames // 4
    quads = [flip(at, axes) for axes in ("y", "z", "yz")]

    def quad_rows(to):
        return aligned((to["z"] // EDGE * 2 + to["y"]) * piece, piece)

    def g_copy(way):
        return remote(g_part.at[:, quad_rows(quads[way]), :], g_recv.at[way], g_ss.at[way], g_rs.at[way], quads[way])

    slot16 = (me * 2 + z // EDGE) * 2 + y

    def p_copy(step):
        return remote(p_send, p_all.at[slot16], p_ss.at[step - 1], p_rs.at[slot16], ahead(at, step))

    @pl.when(edge)
    def _():
        settle(batches - 1)
        for batch in range(batches - 3, batches):
            forward(batch)
        for batch in range(batches):
            spread_copy(me, batch, core_pair, c_ss, c_rs).wait_recv()
            spread_copy(far, batch, core_pair, f_ss, f_rs).wait_recv()
        g_part[...] = jnp.zeros(g_part.shape, F32)

        @pl.loop(0, side)
        def _(col):
            left = y_all[me, col]
            for r in range(g_part.shape[0]):
                g_part[r] += lax.dot_general(left, y_all[r, col], NT, preferred_element_type=F32)

        for way in range(len(quads)):
            g_copy(way).start()
        for way in range(len(quads)):
            g_copy(way).wait_recv()
        power = jnp.zeros(p_send.shape, F32)
        for r in range(g_part.shape[0]):
            gram = g_part[r, quad_rows(at), :]
            for way in range(len(quads)):
                gram = gram + g_recv[way, r]
            power = power + lax.dot_general(gram.astype(BF16), u1_rows[r], NT, preferred_element_type=F32)
        p_send[...] = power
        p_all[slot16] = power
        for step in OTHERS:
            p_copy(step).start()
        for way in range(len(quads)):
            g_copy(way).wait_send()
        for batch in range(batches):
            y_copy(batch).wait_send()
            spread_copy(me, batch, core_pair, c_ss, c_rs).wait_send()
            spread_copy(me, batch, x_pair, w_ss, w_rs).wait_send()
            spread_copy(far, batch, core_pair, f_ss, f_rs).wait_send()

    for source in range(p_all.shape[0]):
        @pl.when(jnp.logical_not(edge) | (slot16 != source))
        def _():
            remote(p_send, p_all.at[source], p_ss.at[0], p_rs.at[source], ahead(at, 1)).wait_recv()

    new_ref[...] = p_all[...] / column_norm(p_all[...], (0, 1))

    @pl.when(edge)
    def _():
        for step in OTHERS:
            p_copy(step).wait_send()

    for slot in range(SLOTS):
        @pl.when(z < last)
        def _():
            link(slot, True).wait_send()

        @pl.when(z > 0)
        def _():
            link(slot, False).wait_send()

    put.wait()
    for way in range(len(partners)):
        swap_copy(way, pl.ds(0, frames)).wait()


def dma(*shape):
    return pltpu.SemaphoreType.DMA(shape)


def first_stage(tensor_t, u3_t, u2_t, u1_t):
    frames, grid_w, grid_h = tensor_t.shape
    half, rank_h, rank_t = u3_t.shape[0] // 2, u2_t.shape[0], u1_t.shape[0]
    link = pltpu.VMEM((SLOTS, half, grid_h), F32)
    any_space = pl.BlockSpec(memory_space=pl.ANY)
    vmem = pl.BlockSpec(memory_space=pltpu.VMEM)
    piece = frames // 4
    groups = grid_w // (4 * TILE)
    return pl.pallas_call(
        first_kernel,
        out_shape=(jax.ShapeDtypeStruct((half // TILE, frames, TILE, grid_h), BF16),
                   jax.ShapeDtypeStruct((4, frames, groups, TILE, grid_h), BF16),
                   jax.ShapeDtypeStruct((16, piece, rank_t), F32)),
        in_specs=[any_space, any_space, vmem, vmem, vmem],
        out_specs=(vmem, any_space, vmem),
        scratch_shapes=[pltpu.VMEM(tensor_t.shape, BF16), pltpu.VMEM((u3_t.shape[0], grid_w), BF16),
                        pltpu.VMEM((rank_h, grid_h), BF16), pltpu.VMEM((4, rank_t, frames), BF16), link, link, link, link,
                        pltpu.VMEM((frames, groups, TILE, grid_h), BF16),
                        pltpu.VMEM((half, frames, rank_h), F32), pltpu.VMEM((half // 2, frames, rank_h), F32),
                        pltpu.VMEM((4, half // 2, frames, rank_h), BF16),
                        pltpu.VMEM((4, frames, frames), F32), pltpu.VMEM((3, 4, piece, frames), F32),
                        pltpu.VMEM((piece, rank_t), F32), pltpu.VMEM((16, piece, rank_t), F32),
                        pltpu.SemaphoreType.REGULAR, pltpu.SemaphoreType.REGULAR, pltpu.SemaphoreType.DMA, pltpu.SemaphoreType.DMA,
                        dma(frames // TILE)] + [dma(SLOTS)] * 4 + [dma(3)] * 2 + [dma(frames // BATCH)] * 8 + [dma(3)] * 2
                       + [dma(COUNT), dma(16)],
        compiler_params=pltpu.CompilerParams(collective_id=1, has_side_effects=True, vmem_limit_bytes=LIMIT),
        name="first_stage",
    )(tensor_t, tensor_t.reshape(frames, grid_w // TILE, TILE, grid_h), u3_t, u2_t, u1_t)


def height_part(at, x_hbm, t_ref, u1_ref, u2_ref, z_out, height_ref, x_slots, kron, y_part, y_core, y_x, y_own, y_other,
                g_part, g_core, g_recv, z_send, p_send, p_all, k_ss, k_rs,
                load_sem, c_ss, c_rs, w_ss, w_rs, y_ss, y_rs, z_ss, z_rs, g_ss, g_rs, p_ss, p_rs):
    barrier = greet(at)
    z, y, x, c = at["z"], at["y"], at["x"], at["c"]
    me = block_of(at)
    edge = (z == 0) | (z == SIZE["z"] - 1)
    blocks, frames, groups, _, grid_h = x_hbm.shape
    rank = u1_ref.shape[1]
    slots = x_slots.shape[0]
    core_pair, x_pair, y_pair = flip(at, "c"), flip(at, "x"), flip(at, "y")

    def load(group):
        slot = lax.rem(group, slots)
        return pltpu.make_async_copy(x_hbm.at[:, :, group], x_slots.at[slot], load_sem.at[slot])

    for group in range(slots):
        load(group).start()
    spread_blocks(rank, u1_ref[...].astype(BF16), at, kron)
    g_part[...] = jnp.zeros(g_part.shape, F32)
    pl.semaphore_wait(barrier, COUNT - 1)

    half, quart = rank // 2, rank // 4

    def core_copy(g):
        return remote(y_part.at[g, pl.ds((1 - c) * half, half)], y_core.at[g], c_ss.at[g], c_rs.at[g], core_pair)

    def wide_copy(g):
        return remote(y_core.at[g, pl.ds((1 - x) * quart, quart)], y_x.at[g], w_ss.at[g], w_rs.at[g], x_pair)

    def tall_copy(g):
        return remote(y_own.at[g], y_other.at[g], y_ss.at[g], y_rs.at[g], y_pair)

    def z_copy(g):
        return remote(z_send.at[g], z_out.at[y, g], z_ss.at[g], z_rs.at[g], y_pair)

    def widen(g):
        core_copy(g).wait_recv()
        y_core[g] += y_part[g, pl.ds(c * half, half)]
        wide_copy(g).start()

    @pl.when(edge)
    def _():
        @pl.loop(0, groups)
        def _(g):
            part = jnp.dot(kron[me], t_ref[g].reshape(frames * TILE, grid_h), preferred_element_type=F32)
            y_part[g] = part.reshape(rank, TILE, grid_h)
            core_copy(g).start()

            @pl.when(g >= 2)
            def _():
                widen(g - 2)

        widen(groups - 2)
        widen(groups - 1)

    def gram(g):
        tall_copy(g).wait_recv()
        left = y_own[g].reshape(quart * TILE, grid_h)
        right = y_other[g].reshape(quart * TILE, grid_h)
        rows = slice(0, grid_h)
        g_part[y, rows, :] += lax.dot_general(left, left, TN, preferred_element_type=F32)
        g_part[1 - y, rows, :] += lax.dot_general(left, right, TN, preferred_element_type=F32)

    @pl.loop(0, groups)
    def _(g):
        load(g).wait()
        slot = lax.rem(g, slots)
        acc = jnp.zeros((rank * TILE, grid_h), F32)
        for block in range(blocks):
            acc = acc + jnp.dot(kron[block], x_slots[slot, block].reshape(frames * TILE, grid_h), preferred_element_type=F32)

        @pl.when(g + slots < groups)
        def _():
            load(g + slots).start()

        whole = acc.reshape(2, half, TILE, grid_h).astype(BF16)
        for index in range(SIZE["y"]):
            @pl.when(y == index)
            def _():
                z_out[index, g] = whole[index]
                z_send[g] = whole[1 - index]

        @pl.when(edge)
        def _():
            wide_copy(g).wait_recv()
            y_own[g] = (y_core[g, pl.ds(x * quart, quart)] + y_x[g]).astype(BF16)
            tall_copy(g).start()

            @pl.when(g >= 2)
            def _():
                gram(g - 2)

        @pl.when(lax.rem(g, 2) == 1)
        def _():
            z_copy(g // 2).start()

    @pl.loop(groups // 2, groups)
    def _(g):
        z_copy(g).start()

    core_rows = g_part.shape[1] // 2
    piece = core_rows // 4
    quads = [flip(at, axes) for axes in ("x", "z", "xz")]

    def k_copy():
        return remote(g_part.at[:, aligned((1 - c) * core_rows, core_rows), :], g_core, k_ss, k_rs, core_pair)

    def quad_rows(to):
        return aligned(c * core_rows + (to["x"] * 2 + to["z"] // EDGE) * piece, piece)

    def g_copy(way):
        return remote(g_part.at[:, quad_rows(quads[way]), :], g_recv.at[way], g_ss.at[way], g_rs.at[way], quads[way])

    slot16 = ((y * 2 + c) * 2 + x) * 2 + z // EDGE

    def p_copy(step):
        return remote(p_send, p_all.at[slot16], p_ss.at[step - 1], p_rs.at[slot16], ahead(at, step))

    @pl.when(edge)
    def _():
        gram(groups - 2)
        gram(groups - 1)
        k_copy().start()
        k_copy().wait_recv()
        g_part[:, aligned(c * core_rows, core_rows), :] += g_core[...]
        for way in range(len(quads)):
            g_copy(way).start()
        for way in range(len(quads)):
            g_copy(way).wait_recv()
        power = jnp.zeros(p_send.shape, F32)
        for r in range(g_part.shape[0]):
            full = g_part[r, quad_rows(at), :]
            for way in range(len(quads)):
                full = full + g_recv[way, r]
            power = power + jnp.dot(full.astype(BF16), u2_ref[r], preferred_element_type=F32)
        p_send[...] = power
        p_all[slot16] = power
        for step in OTHERS:
            p_copy(step).start()
        k_copy().wait_send()
        for way in range(len(quads)):
            g_copy(way).wait_send()

        @pl.loop(0, groups)
        def _(g):
            core_copy(g).wait_send()
            wide_copy(g).wait_send()
            tall_copy(g).wait_send()

    for source in range(p_all.shape[0]):
        @pl.when(jnp.logical_not(edge) | (slot16 != source))
        def _():
            remote(p_send, p_all.at[source], p_ss.at[0], p_rs.at[source], ahead(at, 1)).wait_recv()

    height_ref[...] = p_all[...] / column_norm(p_all[...], (0, 1))

    @pl.when(edge)
    def _():
        for step in OTHERS:
            p_copy(step).wait_send()

    @pl.loop(0, groups)
    def _(g):
        z_copy(g).wait()


def width_part(at, z_ref, height_ref, u3_ref, new_ref, core_ref, energy_ref, u2_cols, y_send, y_recv, y_own, y_line, g_part, g_core, g_quad,
               p_all, q_send, q_all, c_send, c_recv, e_send, e_all,
               a_ss, a_rs, r_ss, l_ss, b_rs, k_ss, k_rs, d_ss, d_rs, q_ss, q_rs, p_ss, p_rs, f_ss, f_rs, n_ss, n_rs, e_ss, e_rs, h_ss, h_rs):
    z, y, x, c = at["z"], at["y"], at["x"], at["c"]
    me = block_of(at)
    mine = member(at, ALL)
    last = SIZE["z"] - 1
    sources, groups, many, eight, grid_h = z_ref.shape
    width = groups * eight
    six = many // 4
    span = 4 * width
    rank_h = height_ref.shape[2]
    side_h = rank_h // 2
    u2_cols[...] = jnp.zeros(u2_cols.shape, BF16)
    for s in range(sources):
        half = height_ref.shape[0] // 2
        rows = height_ref[s * half:(s + 1) * half].reshape(half * height_ref.shape[1], rank_h)[:grid_h]
        cols = rows.T.astype(BF16)
        for side in range(2):
            u2_cols[s, side * PAD:side * PAD + side_h, :] = cols[side * side_h:(side + 1) * side_h]
    for a in range(many):
        acc = jnp.zeros((2 * PAD, width), F32)
        for s in range(sources):
            acc = acc + lax.dot_general(u2_cols[s], z_ref[s, :, a].reshape(width, grid_h), NT, preferred_element_type=F32)
        for side in range(2):
            y_send[a // six, side, (a % six) * PAD:(a % six + 1) * PAD, :] = acc[side * PAD:(side + 1) * PAD].astype(BF16)
    y_recv[me] = y_send[me]
    mates = [flip(at, axes) for axes in ("x", "xc", "c")]

    def quarter_copy(way):
        return remote(y_send.at[block_of(mates[way])], y_recv.at[me], a_ss.at[way], a_rs.at[way], mates[way])

    for way in range(len(mates)):
        quarter_copy(way).start()
    for way in range(len(mates)):
        quarter_copy(way).wait_recv()
    sides = []
    for side in range(2):
        whole = jnp.concatenate([y_recv[q, side].astype(F32) for q in range(4)], axis=1)
        y_own[side] = whole.astype(BF16)
        sides.append(whole)
    y_line[z] = jnp.concatenate(sides, axis=1).astype(BF16)

    right = {**at, "z": jnp.minimum(z + 1, last)}
    left = {**at, "z": jnp.maximum(z - 1, 0)}

    def line_copy(block, to, ss):
        return remote(y_line.at[block], y_line.at[block], ss.at[block], b_rs.at[block], to)

    def pick(values):
        value = values[-1]
        for index in range(last):
            value = jnp.where(z == index, values[index], value)
        return value

    order = [z, pick((1, 0, 1, 2)), pick((2, 2, 3, 1)), pick((3, 3, 0, 0))]
    half_rows = span // 2
    piece = half_rows // 4
    core_pair = flip(at, "c")
    plane = [flip(at, axes) for axes in PLANE]
    quads = [flip(at, axes) for axes in ("x", "y", "yx")]
    ways = range(len(quads))

    def k_copy(block):
        return remote(g_part.at[block, aligned((1 - c) * half_rows, half_rows), :], g_core.at[block], k_ss.at[block], k_rs.at[block], core_pair)

    def quad_rows(to):
        return aligned(c * half_rows + (to["x"] * 2 + to["y"]) * piece, piece)

    def d_copy(block, way):
        return remote(g_part.at[block, quad_rows(quads[way]), :], g_quad.at[way, block], d_ss.at[way, block], d_rs.at[way, block], quads[way])

    def gram(block):
        acc = jnp.zeros((span, span), F32)
        for side in range(2):
            wide = lax.dot_general(y_own[side], y_line[block], TN, preferred_element_type=F32)
            acc = acc + wide[:, side * span:(side + 1) * span]
        g_part[block] = acc
        k_copy(block).start()

    def settle(block):
        k_copy(block).wait_recv()
        g_part[block, aligned(c * half_rows, half_rows), :] += g_core[block]
        for way in ways:
            d_copy(block, way).start()

    def power_of(block):
        full = g_part[block, quad_rows(at), :]
        for way in ways:
            d_copy(block, way).wait_recv()
            full = full + g_quad[way, block]
        return jnp.dot(full.astype(BF16), u3_ref[block], preferred_element_type=F32)

    def pass_on(block):
        @pl.when((block <= z) & (z < last))
        def _():
            line_copy(block, right, r_ss).start()

        @pl.when((block >= z) & (z > 0))
        def _():
            line_copy(block, left, l_ss).start()

    pass_on(z)
    power = jnp.zeros((piece, p_all.shape[3]), F32)
    for k in range(len(order) + 2):
        if k < len(order):
            if k > 0:
                line_copy(order[k], right, r_ss).wait_recv()
                pass_on(order[k])
            gram(order[k])
        if 1 <= k <= len(order):
            settle(order[k - 1])
        if k >= 2:
            power = power + power_of(order[k - 2])

    slot = (c * 2 + x) * 2 + y
    p_all[z, slot] = power
    q_send[...] = jnp.broadcast_to(jnp.sum(power * power, axis=0, keepdims=True), q_send.shape)
    q_all[mine] = q_send[...]

    def q_copy(step):
        return remote(q_send, q_all.at[mine], q_ss.at[step - 1], q_rs.at[COUNT - step - 1], ahead(at, step))

    def rows_copy(owner, ss, rs, to):
        block = p_all.at[owner, slot]
        return remote(block, block, ss, rs, to)

    def p_copy(way):
        return rows_copy(z, p_ss.at[way], p_rs.at[way], plane[way])

    def behind(hop):
        return lax.rem(z + SIZE["z"] - hop, SIZE["z"])

    def n_copy(hop, owner):
        return rows_copy(owner, n_ss.at[hop - 1], n_rs.at[hop - 1], {**at, "z": lax.rem(z + hop, SIZE["z"])})

    def f_copy(way, hop):
        return rows_copy(behind(hop), f_ss.at[way, hop - 1], f_rs.at[way, hop - 1], plane[way])

    hops = range(1, SIZE["z"])
    paths = range(len(plane))
    for step in OTHERS:
        q_copy(step).start()
    for way in paths:
        p_copy(way).start()
    for hop in hops:
        n_copy(hop, z).start()
    for way in paths:
        p_copy(way).wait_recv()
    for step in OTHERS:
        q_copy(step).wait_recv()
    norm = jnp.sqrt(jnp.sum(q_all[:, 0, :], axis=0, keepdims=True))
    factor = (p_all[z].reshape(span, p_all.shape[3]) / norm).astype(BF16)
    fourth = p_all.shape[3] // 4
    for side in range(2):
        part = lax.dot_general(factor, y_own[side], (((0,), (1,)), ((), ())), preferred_element_type=F32)
        for to in range(4):
            c_send[to, side] = part[to * fourth:(to + 1) * fourth]

    zy = z * 2 + y
    c_recv[zy] = c_send[z, y]
    spots = c_recv.shape[0]

    def c_copy(step):
        index = lax.rem(zy + step, spots)
        new = {**at, "z": index // 2, "y": lax.rem(index, 2)}
        return remote(c_send.at[new["z"], new["y"]], c_recv.at[zy], h_ss.at[step - 1], h_rs.at[step - 1], new)

    for step in range(1, spots):
        c_copy(step).start()
    for hop in hops:
        n_copy(hop, behind(hop)).wait_recv()
        for way in paths:
            f_copy(way, hop).start()
    for step in range(1, spots):
        c_copy(step).wait_recv()
    squares = jnp.zeros((1, c_recv.shape[2]), F32)
    for side in range(2):
        full = c_recv[side]
        for source in range(side + 2, spots, 2):
            full = full + c_recv[source]
        core_ref[side] = full
        squares = squares + jnp.sum(full * full, axis=0, keepdims=True)
    e_send[...] = jnp.broadcast_to(jnp.sum(squares, axis=1, keepdims=True), e_send.shape)
    e_all[mine] = e_send[...]

    def e_copy(step):
        return remote(e_send, e_all.at[mine], e_ss.at[step - 1], e_rs.at[COUNT - step - 1], ahead(at, step))

    for step in OTHERS:
        e_copy(step).start()
    for hop in hops:
        for way in paths:
            f_copy(way, hop).wait_recv()
    new_ref[...] = p_all[...] / norm[None, None]
    for step in OTHERS:
        e_copy(step).wait_recv()
    energy_ref[...] = jnp.sum(e_all[...], axis=0)

    for way in range(len(mates)):
        quarter_copy(way).wait_send()
    for block in order:
        @pl.when((block <= z) & (z < last))
        def _():
            line_copy(block, right, r_ss).wait_send()

        @pl.when((block >= z) & (z > 0))
        def _():
            line_copy(block, left, l_ss).wait_send()

        k_copy(block).wait_send()
        for way in ways:
            d_copy(block, way).wait_send()
    for step in OTHERS:
        q_copy(step).wait_send()
        e_copy(step).wait_send()
    for way in paths:
        p_copy(way).wait_send()
        for hop in hops:
            f_copy(way, hop).wait_send()
    for hop in hops:
        n_copy(hop, z).wait_send()
    for step in range(1, spots):
        c_copy(step).wait_send()


HEIGHT_SCRATCH = 28


def second_kernel(x_hbm, t_ref, u1_ref, u2_ref, u3_ref, height_ref, new_ref, core_ref, energy_ref, z_all, *scratch):
    at = place()
    height_part(at, x_hbm, t_ref, u1_ref, u2_ref, z_all, height_ref, *scratch[:HEIGHT_SCRATCH])
    width_part(at, z_all, height_ref, u3_ref, new_ref, core_ref, energy_ref, *scratch[HEIGHT_SCRATCH:])


def second_stage(x_all, t_mat, new_time, u2, u3):
    blocks, frames, groups, _, grid_h = x_all.shape
    rank, rank_h, rank_w = new_time.shape[1], u2.shape[1], u3.shape[1]
    vmem = pl.BlockSpec(memory_space=pltpu.VMEM)
    rows = 384
    piece = rows // TILE
    width = groups * TILE
    cols = rank // TILE * PAD
    small = width // 2
    fourth = rank_w // 4

    def f32(*shape):
        return pltpu.VMEM(shape, F32)

    def bf16(*shape):
        return pltpu.VMEM(shape, BF16)

    one = pltpu.SemaphoreType.DMA
    height = [bf16(4, blocks, frames, TILE, grid_h), bf16(blocks, rank * TILE, frames * TILE),
              f32(groups, rank, TILE, grid_h), f32(groups, rank // 2, TILE, grid_h), f32(groups, rank // 4, TILE, grid_h),
              bf16(groups, rank // 4, TILE, grid_h), bf16(groups, rank // 4, TILE, grid_h),
              f32(2, rows, grid_h), f32(2, rows // 2, grid_h), f32(3, 2, piece, grid_h),
              bf16(groups, rank // 2, TILE, grid_h), f32(piece, rank_h), f32(16, piece, rank_h), one, one,
              dma(4)] + [dma(groups)] * 8 + [dma(3), dma(3), dma(COUNT), dma(16)]
    wide = [bf16(2, 2 * PAD, grid_h), bf16(4, 2, cols, width), bf16(4, 2, cols, width), bf16(2, cols, 4 * width), bf16(4, cols, 2 * 4 * width),
            f32(4, 4 * width, 4 * width), f32(4, 2 * width, 4 * width), f32(3, 4, small, 4 * width),
            f32(4, 2 * 4, small, rank_w), f32(TILE, rank_w), f32(COUNT, TILE, rank_w),
            f32(4, 2, fourth, cols), f32(2 * 4, fourth, cols), f32(TILE, 128), f32(COUNT, TILE, 128),
            dma(3), dma(3)] + [dma(4)] * 5 + [dma(3, 4), dma(3, 4), dma(COUNT), dma(COUNT)] + [dma(7)] * 2 + [dma(7, 3)] * 2 + [dma(3)] * 2 \
        + [dma(COUNT)] * 2 + [dma(7)] * 2
    return pl.pallas_call(
        second_kernel,
        out_shape=(jax.ShapeDtypeStruct((16, piece, rank_h), F32),
                   jax.ShapeDtypeStruct((4, 2 * 4, small, rank_w), F32),
                   jax.ShapeDtypeStruct((2, fourth, cols), F32),
                   jax.ShapeDtypeStruct((TILE, 128), F32)),
        in_specs=[pl.BlockSpec(memory_space=pl.ANY), vmem, vmem, vmem, vmem],
        out_specs=(vmem, vmem, vmem, vmem),
        scratch_shapes=[bf16(2, groups, rank // 2, TILE, grid_h)] + height + wide,
        compiler_params=pltpu.CompilerParams(collective_id=2, has_side_effects=True, vmem_limit_bytes=LIMIT),
        name="second_stage",
    )(x_all, t_mat, new_time, u2.astype(BF16).reshape(2, grid_h, rank_h), u3.astype(BF16).reshape(4, 4 * width, rank_w))


def solution(mesh):
    def local_sweep(tensor, u_time, u_height, u_width):
        frames, grid_h, grid_w = tensor.shape
        rank_t, rank_h, rank_w = u_time.shape[1], u_height.shape[1], u_width.shape[1]
        t_mat, x_all, new_time = first_stage(tensor.swapaxes(1, 2), u_width.T, u_height.T, u_time.T)
        new_time = new_time.reshape(-1, rank_t)
        power, new_width, core, energy = second_stage(x_all, t_mat, new_time, u_height, u_width)
        new_height = power.reshape(2, -1, rank_h)[:, :grid_h].reshape(-1, rank_h)
        new_width = new_width.reshape(-1, rank_w)
        core = core.reshape(2, rank_w // 4, rank_t // 8, PAD)[..., :rank_h // 2].transpose(0, 2, 3, 1)
        core_tensor = core.reshape(rank_t // 4, rank_h // 2, rank_w // 4)
        return new_time, new_height, new_width, core_tensor, energy[0, 0]

    return jax.shard_map(local_sweep, mesh=mesh, in_specs=(P("a1", "a2", "a3"), P(), P(), P()), out_specs=(P(), P(), P(), P("a1", "a2", "a3"), P()), check_vma=False)
```

```python
import jax
import jax.numpy as jnp
from jax import lax
from jax.experimental import pallas as pl
from jax.experimental.pallas import tpu as pltpu
from jax.sharding import PartitionSpec as P

MESH = pl.DeviceIdType.MESH
F32 = jnp.float32
BF16 = jnp.bfloat16
SIZE = {"z": 4, "y": 2, "x": 2, "c": 2}
ALL = ("z", "y", "x", "c")
COUNT = 32
OTHERS = range(1, COUNT)
PLANE = ("c", "x", "y", "xc", "yc", "yx", "yxc")
LAG = 2
SLOTS = 8
BATCH = 16
TILE = 8
PAD = 48
EDGE = 3
NT = (((1,), (1,)), ((), ()))
TN = (((0,), (0,)), ((), ()))
LIMIT = 60 * 1024 * 1024


def place():
    a1 = lax.axis_index("a1")
    return {"z": lax.axis_index("a3"), "y": lax.axis_index("a2"), "x": a1 // 2, "c": lax.rem(a1, 2)}


def device(at):
    return (at["z"], at["y"], at["x"] * 2 + at["c"])


def block_of(at):
    return at["x"] * 2 + at["c"]


def member(at, group):
    index = 0
    for axis in group:
        index = index * SIZE[axis] + at[axis]
    return index


def flip(at, axes):
    return {axis: SIZE[axis] - 1 - at[axis] if axis in axes else at[axis] for axis in at}


def ahead(at, step):
    index = lax.rem(member(at, ALL) + step, COUNT)
    new = {}
    for axis in reversed(ALL):
        new[axis] = lax.rem(index, SIZE[axis])
        index = index // SIZE[axis]
    return new


def remote(src, dst, ss, rs, to):
    return pltpu.make_async_remote_copy(src_ref=src, dst_ref=dst, send_sem=ss, recv_sem=rs, device_id=device(to), device_id_type=MESH)


def greet(at):
    barrier = pltpu.get_barrier_semaphore()
    for step in OTHERS:
        pl.semaphore_signal(barrier, inc=1, device_id=device(ahead(at, step)), device_id_type=MESH)
    return barrier


def aligned(start, size):
    return pl.ds(pl.multiple_of(start, TILE), size)


def column_norm(power, axes):
    return jnp.sqrt(jnp.sum(power * power, axis=axes, keepdims=True))


def eights(shape, axis):
    return lax.broadcasted_iota(jnp.int32, shape, axis) // TILE


def in_eight(shape, axis):
    return lax.rem(lax.broadcasted_iota(jnp.int32, shape, axis), TILE)


def spread_blocks(rank, values, at, kron):
    blocks, _, width = kron.shape
    shape = (rank * TILE, rank)
    row = eights(shape, 0)
    sixth = rank // TILE
    quarter = row // sixth
    wanted = (lax.rem(quarter, 4) * 2 + quarter // 4) * sixth + lax.rem(row, sixth)
    picks = jnp.where(lax.broadcasted_iota(jnp.int32, shape, 1) == wanted, 1.0, 0.0).astype(BF16)
    spread = lax.dot_general(picks, values, NT, preferred_element_type=F32).astype(BF16)
    for block in range(blocks):
        shape = (values.shape[0], width)
        match = eights(shape, 1) + block * (width // TILE) == lax.broadcasted_iota(jnp.int32, shape, 0)
        wide = jnp.dot(spread, jnp.where(match, 1.0, 0.0).astype(BF16), preferred_element_type=F32)
        same = in_eight(wide.shape, 0) == in_eight(wide.shape, 1)
        kron[block] = jnp.where(same, wide, 0.0).astype(BF16)


def first_kernel(x_hbm, x_tiles, u3_ref, u2_ref, u1_ref, t_ref, x_all, new_ref, x_vmem, u3_rows, u2_rows, u1_rows, s_up, r_up, s_dn, r_dn,
                 own_tiles, y_part, y_recv, y_all, g_part, g_recv, p_send, p_all, free_up, free_dn, own_in, own_sem,
                 load_sem, ss_up, rs_up, ss_dn, rs_dn, x_send, x_recv,
                 y_ss, y_rs, c_ss, c_rs, w_ss, w_rs, f_ss, f_rs, g_ss, g_rs, p_ss, p_rs):
    frames, grid_w, grid_h = x_hbm.shape
    at = place()
    z, y = at["z"], at["y"]
    me = block_of(at)
    half = t_ref.shape[0] * TILE
    groups = x_all.shape[2]
    last = SIZE["z"] - 1
    edge = (z == 0) | (z == last)
    for part in range(frames // TILE):
        rows = pl.ds(part * TILE, TILE)
        pltpu.make_async_copy(x_hbm.at[rows], x_vmem.at[rows], load_sem.at[part]).start()
    barrier = greet(at)
    own = pltpu.make_async_copy(x_tiles.at[:, pl.ds(me * groups, groups)], own_tiles, own_in)
    own.start()
    for index in range(SIZE["z"]):
        @pl.when(z == index)
        def _():
            u3_rows[...] = u3_ref[:, index * grid_w:(index + 1) * grid_w].astype(BF16)

    for index in range(SIZE["y"]):
        @pl.when(y == index)
        def _():
            u2_rows[...] = u2_ref[:, index * grid_h:(index + 1) * grid_h].astype(BF16)

    u1_rows[...] = u1_ref[...].astype(BF16)

    @pl.when(jnp.logical_not(edge))
    def _():
        @pl.loop(0, frames)
        def _(frame):
            t_ref[:, frame] = jnp.zeros((half // TILE, TILE, grid_h), BF16)

    pl.semaphore_wait(barrier, COUNT - 1)

    core_pair, x_pair, y_pair = flip(at, "c"), flip(at, "x"), flip(at, "y")
    partners = [core_pair, x_pair, flip(at, "xc")]

    def swap_copy(way, frame):
        new = partners[way]
        return remote(x_tiles.at[frame, pl.ds(block_of(new) * groups, groups)], x_all.at[me, frame], x_send.at[way], x_recv.at[way], new)

    def link(slot, up):
        if up:
            return remote(s_up.at[slot], r_up.at[slot], ss_up.at[slot], rs_up.at[slot], {**at, "z": above})
        return remote(s_dn.at[slot], r_dn.at[slot], ss_dn.at[slot], rs_dn.at[slot], {**at, "z": below})

    def stream(frame, up):
        start, end, back, factor = (0, last, below, u3_rows[half:]) if up else (last, 0, above, u3_rows[:half])
        sends, recvs, free = (s_up, r_up, free_up) if up else (s_dn, r_dn, free_dn)

        @pl.when((frame >= 0) & (frame < frames))
        def _():
            slot = lax.rem(frame, SLOTS)
            copy = link(slot, up)
            part = jnp.dot(factor, x_vmem[frame], preferred_element_type=F32)

            @pl.when((z != end) & (frame >= SLOTS))
            def _():
                copy.wait_send()
                pl.semaphore_wait(free, 1)

            sends[slot] = part

            @pl.when(z != start)
            def _():
                copy.wait_recv()
                sends[slot] += recvs[slot]

                @pl.when(frame + SLOTS < frames)
                def _():
                    pl.semaphore_signal(free, inc=1, device_id=device({**at, "z": back}), device_id_type=MESH)

            @pl.when(z != end)
            def _():
                copy.start()

            @pl.when(z == end)
            def _():
                done = sends[slot].astype(BF16)
                t_ref[:, frame] = done.reshape(half // TILE, TILE, grid_h)
                rows = lax.dot_general(done, u2_rows[...], NT, preferred_element_type=F32)
                y_part[:, pl.ds(frame, 1), :] = rows[:, None, :]

    side = half // 2
    keep, give = pl.ds(y * side, side), pl.ds((1 - y) * side, side)

    def rows_at(batch):
        return pl.ds(pl.multiple_of(batch * BATCH, BATCH), BATCH)

    def y_copy(batch):
        rows = rows_at(batch)
        return remote(y_part.at[give, rows, :], y_recv.at[:, rows, :], y_ss.at[batch], y_rs.at[batch], y_pair)

    def spread_copy(owner, batch, pair, ss, rs):
        block = y_all.at[owner, :, rows_at(batch), :]
        return remote(block, block, ss.at[batch], rs.at[batch], pair)

    far = block_of(x_pair)

    def settle(batch):
        y_copy(batch).wait_recv()
        rows = rows_at(batch)
        y_all[me, :, rows, :] = (y_part[keep, rows, :] + y_recv[:, rows, :]).astype(BF16)
        spread_copy(me, batch, core_pair, c_ss, c_rs).start()
        spread_copy(me, batch, x_pair, w_ss, w_rs).start()

    def forward(batch):
        spread_copy(me, batch, x_pair, w_ss, w_rs).wait_recv()
        spread_copy(far, batch, core_pair, f_ss, f_rs).start()

    own.wait()
    put = pltpu.make_async_copy(own_tiles, x_all.at[me], own_sem)
    put.start()
    above = jnp.minimum(z + 1, last)
    below = jnp.maximum(z - 1, 0)
    lead = jnp.minimum(z, last - z)

    @pl.loop(0, frames + last * LAG)
    def _(step):
        newest = step - LAG * lead

        @pl.when(step < frames)
        def _():
            for way in range(len(partners)):
                swap_copy(way, jnp.minimum(step, frames - 1)).start()

        @pl.when((newest >= 0) & (newest < frames) & (lax.rem(newest, TILE) == 0))
        def _():
            part = newest // TILE
            rows = aligned(part * TILE, TILE)
            pltpu.make_async_copy(x_hbm.at[rows], x_vmem.at[rows], load_sem.at[part]).wait()

        stream(step - LAG * z, True)
        stream(step - LAG * (last - z), False)
        final = step - last * LAG

        @pl.when(edge & (final >= 0))
        def _():
            place_in = lax.rem(final, BATCH)
            batch = final // BATCH

            @pl.when(place_in == BATCH - 1)
            def _():
                y_copy(batch).start()

            @pl.when((place_in == BATCH // 2) & (batch >= 1))
            def _():
                settle(batch - 1)

            @pl.when((place_in == BATCH // 2) & (batch >= 3))
            def _():
                forward(batch - 3)

    batches = frames // BATCH
    piece = frames // 4
    quads = [flip(at, axes) for axes in ("y", "z", "yz")]

    def quad_rows(to):
        return aligned((to["z"] // EDGE * 2 + to["y"]) * piece, piece)

    def g_copy(way):
        return remote(g_part.at[quad_rows(quads[way]), :], g_recv.at[way], g_ss.at[way], g_rs.at[way], quads[way])

    slot16 = (me * 2 + z // EDGE) * 2 + y

    def p_copy(step):
        return remote(p_send, p_all.at[slot16], p_ss.at[step - 1], p_rs.at[slot16], ahead(at, step))

    @pl.when(edge)
    def _():
        settle(batches - 1)
        for batch in range(batches - 3, batches):
            forward(batch)
        for batch in range(batches):
            spread_copy(me, batch, core_pair, c_ss, c_rs).wait_recv()
            spread_copy(far, batch, core_pair, f_ss, f_rs).wait_recv()
        g_part[...] = jnp.zeros(g_part.shape, F32)

        @pl.loop(0, side // 4)
        def _(four):
            acc = g_part[...]
            for step in range(4):
                col = four * 4 + step
                right = y_all[:, col].reshape(y_all.shape[0] * frames, y_all.shape[3])
                acc = acc + lax.dot_general(y_all[me, col], right, NT, preferred_element_type=F32)
            g_part[...] = acc

        for way in range(len(quads)):
            g_copy(way).start()
        for way in range(len(quads)):
            g_copy(way).wait_recv()
        gram = g_part[quad_rows(at), :]
        for way in range(len(quads)):
            gram = gram + g_recv[way]
        power = lax.dot_general(gram.astype(BF16), u1_rows[...], NT, preferred_element_type=F32)
        p_send[...] = power
        p_all[slot16] = power
        for step in OTHERS:
            p_copy(step).start()
        for way in range(len(quads)):
            g_copy(way).wait_send()
        for batch in range(batches):
            y_copy(batch).wait_send()
            spread_copy(me, batch, core_pair, c_ss, c_rs).wait_send()
            spread_copy(me, batch, x_pair, w_ss, w_rs).wait_send()
            spread_copy(far, batch, core_pair, f_ss, f_rs).wait_send()

    for source in range(p_all.shape[0]):
        @pl.when(jnp.logical_not(edge) | (slot16 != source))
        def _():
            remote(p_send, p_all.at[source], p_ss.at[0], p_rs.at[source], ahead(at, 1)).wait_recv()

    new_ref[...] = p_all[...] / column_norm(p_all[...], (0, 1))

    @pl.when(edge)
    def _():
        for step in OTHERS:
            p_copy(step).wait_send()

    for slot in range(SLOTS):
        @pl.when(z < last)
        def _():
            link(slot, True).wait_send()

        @pl.when(z > 0)
        def _():
            link(slot, False).wait_send()

    put.wait()
    for way in range(len(partners)):
        swap_copy(way, pl.ds(0, frames)).wait()


def dma(*shape):
    return pltpu.SemaphoreType.DMA(shape)


def first_stage(tensor_t, u3_t, u2_t, u1_t):
    frames, grid_w, grid_h = tensor_t.shape
    half, rank_h, rank_t = u3_t.shape[0] // 2, u2_t.shape[0], u1_t.shape[0]
    link = pltpu.VMEM((SLOTS, half, grid_h), F32)
    any_space = pl.BlockSpec(memory_space=pl.ANY)
    vmem = pl.BlockSpec(memory_space=pltpu.VMEM)
    piece = frames // 4
    groups = grid_w // (4 * TILE)
    return pl.pallas_call(
        first_kernel,
        out_shape=(jax.ShapeDtypeStruct((half // TILE, frames, TILE, grid_h), BF16),
                   jax.ShapeDtypeStruct((4, frames, groups, TILE, grid_h), BF16),
                   jax.ShapeDtypeStruct((16, piece, rank_t), F32)),
        in_specs=[any_space, any_space, vmem, vmem, vmem],
        out_specs=(vmem, any_space, vmem),
        scratch_shapes=[pltpu.VMEM(tensor_t.shape, BF16), pltpu.VMEM((u3_t.shape[0], grid_w), BF16),
                        pltpu.VMEM((rank_h, grid_h), BF16), pltpu.VMEM((rank_t, 4 * frames), BF16), link, link, link, link,
                        pltpu.VMEM((frames, groups, TILE, grid_h), BF16),
                        pltpu.VMEM((half, frames, rank_h), F32), pltpu.VMEM((half // 2, frames, rank_h), F32),
                        pltpu.VMEM((4, half // 2, frames, rank_h), BF16),
                        pltpu.VMEM((frames, 4 * frames), F32), pltpu.VMEM((3, piece, 4 * frames), F32),
                        pltpu.VMEM((piece, rank_t), F32), pltpu.VMEM((16, piece, rank_t), F32),
                        pltpu.SemaphoreType.REGULAR, pltpu.SemaphoreType.REGULAR, pltpu.SemaphoreType.DMA, pltpu.SemaphoreType.DMA,
                        dma(frames // TILE)] + [dma(SLOTS)] * 4 + [dma(3)] * 2 + [dma(frames // BATCH)] * 8 + [dma(3)] * 2
                       + [dma(COUNT), dma(16)],
        compiler_params=pltpu.CompilerParams(collective_id=1, has_side_effects=True, vmem_limit_bytes=LIMIT),
        name="first_stage",
    )(tensor_t, tensor_t.reshape(frames, grid_w // TILE, TILE, grid_h), u3_t, u2_t, u1_t)


def height_part(at, x_hbm, t_ref, u1_ref, u2_ref, z_out, height_ref, x_slots, kron, y_part, y_core, y_x, y_own, y_other,
                g_part, g_core, g_recv, z_send, p_send, p_all, k_ss, k_rs,
                load_sem, c_ss, c_rs, w_ss, w_rs, y_ss, y_rs, z_ss, z_rs, g_ss, g_rs, p_ss, p_rs):
    barrier = greet(at)
    z, y, x, c = at["z"], at["y"], at["x"], at["c"]
    me = block_of(at)
    edge = (z == 0) | (z == SIZE["z"] - 1)
    blocks, frames, groups, _, grid_h = x_hbm.shape
    rank = u1_ref.shape[1]
    slots = x_slots.shape[0]
    core_pair, x_pair, y_pair = flip(at, "c"), flip(at, "x"), flip(at, "y")

    def load(group):
        slot = lax.rem(group, slots)
        return pltpu.make_async_copy(x_hbm.at[:, :, group], x_slots.at[slot], load_sem.at[slot])

    for group in range(slots):
        load(group).start()
    spread_blocks(rank, u1_ref[...].astype(BF16), at, kron)
    g_part[...] = jnp.zeros(g_part.shape, F32)
    pl.semaphore_wait(barrier, COUNT - 1)

    half, quart = rank // 2, rank // 4

    def core_copy(g):
        return remote(y_part.at[g, pl.ds((1 - c) * half, half)], y_core.at[g], c_ss.at[g], c_rs.at[g], core_pair)

    def wide_copy(g):
        return remote(y_core.at[g, pl.ds((1 - x) * quart, quart)], y_x.at[g], w_ss.at[g], w_rs.at[g], x_pair)

    def tall_copy(g):
        return remote(y_own.at[g], y_other.at[g], y_ss.at[g], y_rs.at[g], y_pair)

    def z_copy(g):
        return remote(z_send.at[g], z_out.at[y, g], z_ss.at[g], z_rs.at[g], y_pair)

    def widen(g):
        core_copy(g).wait_recv()
        y_core[g] += y_part[g, pl.ds(c * half, half)]
        wide_copy(g).start()

    @pl.when(edge)
    def _():
        @pl.loop(0, groups)
        def _(g):
            part = jnp.dot(kron[me], t_ref[g].reshape(frames * TILE, grid_h), preferred_element_type=F32)
            y_part[g] = part.reshape(rank, TILE, grid_h)
            core_copy(g).start()

            @pl.when(g >= 2)
            def _():
                widen(g - 2)

        widen(groups - 2)
        widen(groups - 1)

    def gram(g):
        tall_copy(g).wait_recv()
        left = y_own[g].reshape(quart * TILE, grid_h)
        right = y_other[g].reshape(quart * TILE, grid_h)
        rows = slice(0, grid_h)
        g_part[y, rows, :] += lax.dot_general(left, left, TN, preferred_element_type=F32)
        g_part[1 - y, rows, :] += lax.dot_general(left, right, TN, preferred_element_type=F32)

    @pl.loop(0, groups)
    def _(g):
        load(g).wait()
        slot = lax.rem(g, slots)
        acc = jnp.zeros((rank * TILE, grid_h), F32)
        for block in range(blocks):
            acc = acc + jnp.dot(kron[block], x_slots[slot, block].reshape(frames * TILE, grid_h), preferred_element_type=F32)

        @pl.when(g + slots < groups)
        def _():
            load(g + slots).start()

        whole = acc.reshape(2, half, TILE, grid_h).astype(BF16)
        for index in range(SIZE["y"]):
            @pl.when(y == index)
            def _():
                z_out[index, g] = whole[index]
                z_send[g] = whole[1 - index]

        @pl.when(edge)
        def _():
            wide_copy(g).wait_recv()
            y_own[g] = (y_core[g, pl.ds(x * quart, quart)] + y_x[g]).astype(BF16)
            tall_copy(g).start()

            @pl.when(g >= 2)
            def _():
                gram(g - 2)

        @pl.when(lax.rem(g, 2) == 1)
        def _():
            z_copy(g // 2).start()

    @pl.loop(groups // 2, groups)
    def _(g):
        z_copy(g).start()

    core_rows = g_part.shape[1] // 2
    piece = core_rows // 4
    quads = [flip(at, axes) for axes in ("x", "z", "xz")]

    def k_copy():
        return remote(g_part.at[:, aligned((1 - c) * core_rows, core_rows), :], g_core, k_ss, k_rs, core_pair)

    def quad_rows(to):
        return aligned(c * core_rows + (to["x"] * 2 + to["z"] // EDGE) * piece, piece)

    def g_copy(way):
        return remote(g_part.at[:, quad_rows(quads[way]), :], g_recv.at[way], g_ss.at[way], g_rs.at[way], quads[way])

    slot16 = ((y * 2 + c) * 2 + x) * 2 + z // EDGE

    def p_copy(step):
        return remote(p_send, p_all.at[slot16], p_ss.at[step - 1], p_rs.at[slot16], ahead(at, step))

    @pl.when(edge)
    def _():
        gram(groups - 2)
        gram(groups - 1)
        k_copy().start()
        k_copy().wait_recv()
        g_part[:, aligned(c * core_rows, core_rows), :] += g_core[...]
        for way in range(len(quads)):
            g_copy(way).start()
        for way in range(len(quads)):
            g_copy(way).wait_recv()
        power = jnp.zeros(p_send.shape, F32)
        for r in range(g_part.shape[0]):
            full = g_part[r, quad_rows(at), :]
            for way in range(len(quads)):
                full = full + g_recv[way, r]
            rows = u2_ref[:, r * grid_h:(r + 1) * grid_h].astype(BF16)
            power = power + lax.dot_general(full.astype(BF16), rows, NT, preferred_element_type=F32)
        p_send[...] = power
        p_all[slot16] = power
        for step in OTHERS:
            p_copy(step).start()
        k_copy().wait_send()
        for way in range(len(quads)):
            g_copy(way).wait_send()

        @pl.loop(0, groups)
        def _(g):
            core_copy(g).wait_send()
            wide_copy(g).wait_send()
            tall_copy(g).wait_send()

    for source in range(p_all.shape[0]):
        @pl.when(jnp.logical_not(edge) | (slot16 != source))
        def _():
            remote(p_send, p_all.at[source], p_ss.at[0], p_rs.at[source], ahead(at, 1)).wait_recv()

    height_ref[...] = p_all[...] / column_norm(p_all[...], (0, 1))

    @pl.when(edge)
    def _():
        for step in OTHERS:
            p_copy(step).wait_send()

    @pl.loop(0, groups)
    def _(g):
        z_copy(g).wait()


def width_part(at, z_ref, height_ref, u3_ref, new_ref, core_ref, energy_ref, u3_rows, u2_cols, y_send, y_recv, y_own, y_line, g_part, g_core, g_quad,
               p_all, q_send, q_all, c_send, c_recv, e_send, e_all,
               a_ss, a_rs, r_ss, l_ss, b_rs, k_ss, k_rs, d_ss, d_rs, q_ss, q_rs, p_ss, p_rs, f_ss, f_rs, n_ss, n_rs, e_ss, e_rs, h_ss, h_rs):
    z, y, x, c = at["z"], at["y"], at["x"], at["c"]
    me = block_of(at)
    mine = member(at, ALL)
    last = SIZE["z"] - 1
    sources, groups, many, eight, grid_h = z_ref.shape
    width = groups * eight
    six = many // 4
    span = 4 * width
    rank_h = height_ref.shape[2]
    side_h = rank_h // 2
    for index in range(SIZE["z"]):
        u3_rows[index] = u3_ref[:, index * span:(index + 1) * span].astype(BF16)
    u2_cols[...] = jnp.zeros(u2_cols.shape, BF16)
    for s in range(sources):
        half = height_ref.shape[0] // 2
        rows = height_ref[s * half:(s + 1) * half].reshape(half * height_ref.shape[1], rank_h)[:grid_h]
        cols = rows.T.astype(BF16)
        for side in range(2):
            u2_cols[s, side * PAD:side * PAD + side_h, :] = cols[side * side_h:(side + 1) * side_h]
    for a in range(many):
        acc = jnp.zeros((2 * PAD, width), F32)
        for s in range(sources):
            acc = acc + lax.dot_general(u2_cols[s], z_ref[s, :, a].reshape(width, grid_h), NT, preferred_element_type=F32)
        for side in range(2):
            y_send[a // six, side, (a % six) * PAD:(a % six + 1) * PAD, :] = acc[side * PAD:(side + 1) * PAD].astype(BF16)
    y_recv[me] = y_send[me]
    mates = [flip(at, axes) for axes in ("x", "xc", "c")]

    def quarter_copy(way):
        return remote(y_send.at[block_of(mates[way])], y_recv.at[me], a_ss.at[way], a_rs.at[way], mates[way])

    for way in range(len(mates)):
        quarter_copy(way).start()
    for way in range(len(mates)):
        quarter_copy(way).wait_recv()
    sides = []
    for side in range(2):
        whole = jnp.concatenate([y_recv[q, side].astype(F32) for q in range(4)], axis=1)
        y_own[side] = whole.astype(BF16)
        sides.append(whole)
    y_line[z] = jnp.concatenate(sides, axis=1).astype(BF16)

    right = {**at, "z": jnp.minimum(z + 1, last)}
    left = {**at, "z": jnp.maximum(z - 1, 0)}

    def line_copy(block, to, ss):
        return remote(y_line.at[block], y_line.at[block], ss.at[block], b_rs.at[block], to)

    def pick(values):
        value = values[-1]
        for index in range(last):
            value = jnp.where(z == index, values[index], value)
        return value

    order = [z, pick((1, 0, 1, 2)), pick((2, 2, 3, 1)), pick((3, 3, 0, 0))]
    half_rows = span // 2
    piece = half_rows // 4
    core_pair = flip(at, "c")
    plane = [flip(at, axes) for axes in PLANE]
    quads = [flip(at, axes) for axes in ("x", "y", "yx")]
    ways = range(len(quads))

    def k_copy(block):
        return remote(g_part.at[block, aligned((1 - c) * half_rows, half_rows), :], g_core.at[block], k_ss.at[block], k_rs.at[block], core_pair)

    def quad_rows(to):
        return aligned(c * half_rows + (to["x"] * 2 + to["y"]) * piece, piece)

    def d_copy(block, way):
        return remote(g_part.at[block, quad_rows(quads[way]), :], g_quad.at[way, block], d_ss.at[way, block], d_rs.at[way, block], quads[way])

    def gram(block):
        acc = jnp.zeros((span, span), F32)
        for side in range(2):
            wide = lax.dot_general(y_own[side], y_line[block], TN, preferred_element_type=F32)
            acc = acc + wide[:, side * span:(side + 1) * span]
        g_part[block] = acc
        k_copy(block).start()

    def settle(block):
        k_copy(block).wait_recv()
        g_part[block, aligned(c * half_rows, half_rows), :] += g_core[block]
        for way in ways:
            d_copy(block, way).start()

    def power_of(block):
        full = g_part[block, quad_rows(at), :]
        for way in ways:
            d_copy(block, way).wait_recv()
            full = full + g_quad[way, block]
        return lax.dot_general(full.astype(BF16), u3_rows[block], NT, preferred_element_type=F32)

    def pass_on(block):
        @pl.when((block <= z) & (z < last))
        def _():
            line_copy(block, right, r_ss).start()

        @pl.when((block >= z) & (z > 0))
        def _():
            line_copy(block, left, l_ss).start()

    pass_on(z)
    power = jnp.zeros((piece, p_all.shape[3]), F32)
    for k in range(len(order) + 2):
        if k < len(order):
            if k > 0:
                line_copy(order[k], right, r_ss).wait_recv()
                pass_on(order[k])
            gram(order[k])
        if 1 <= k <= len(order):
            settle(order[k - 1])
        if k >= 2:
            power = power + power_of(order[k - 2])

    slot = (c * 2 + x) * 2 + y
    p_all[z, slot] = power
    q_send[...] = jnp.broadcast_to(jnp.sum(power * power, axis=0, keepdims=True), q_send.shape)
    q_all[mine] = q_send[...]

    def q_copy(step):
        return remote(q_send, q_all.at[mine], q_ss.at[step - 1], q_rs.at[COUNT - step - 1], ahead(at, step))

    def rows_copy(owner, ss, rs, to):
        block = p_all.at[owner, slot]
        return remote(block, block, ss, rs, to)

    def p_copy(way):
        return rows_copy(z, p_ss.at[way], p_rs.at[way], plane[way])

    def behind(hop):
        return lax.rem(z + SIZE["z"] - hop, SIZE["z"])

    def n_copy(hop, owner):
        return rows_copy(owner, n_ss.at[hop - 1], n_rs.at[hop - 1], {**at, "z": lax.rem(z + hop, SIZE["z"])})

    def f_copy(way, hop):
        return rows_copy(behind(hop), f_ss.at[way, hop - 1], f_rs.at[way, hop - 1], plane[way])

    hops = range(1, SIZE["z"])
    paths = range(len(plane))
    for step in OTHERS:
        q_copy(step).start()
    for way in paths:
        p_copy(way).start()
    for hop in hops:
        n_copy(hop, z).start()
    for way in paths:
        p_copy(way).wait_recv()
    for step in OTHERS:
        q_copy(step).wait_recv()
    norm = jnp.sqrt(jnp.sum(q_all[:, 0, :], axis=0, keepdims=True))
    factor = (p_all[z].reshape(span, p_all.shape[3]) / norm).astype(BF16)
    fourth = p_all.shape[3] // 4
    for side in range(2):
        part = lax.dot_general(factor, y_own[side], (((0,), (1,)), ((), ())), preferred_element_type=F32)
        for to in range(4):
            c_send[to, side] = part[to * fourth:(to + 1) * fourth]

    zy = z * 2 + y
    c_recv[zy] = c_send[z, y]
    spots = c_recv.shape[0]

    def c_copy(step):
        index = lax.rem(zy + step, spots)
        new = {**at, "z": index // 2, "y": lax.rem(index, 2)}
        return remote(c_send.at[new["z"], new["y"]], c_recv.at[zy], h_ss.at[step - 1], h_rs.at[step - 1], new)

    for step in range(1, spots):
        c_copy(step).start()
    for hop in hops:
        n_copy(hop, behind(hop)).wait_recv()
        for way in paths:
            f_copy(way, hop).start()
    for step in range(1, spots):
        c_copy(step).wait_recv()
    squares = jnp.zeros((1, c_recv.shape[2]), F32)
    for side in range(2):
        full = c_recv[side]
        for source in range(side + 2, spots, 2):
            full = full + c_recv[source]
        core_ref[side] = full
        squares = squares + jnp.sum(full * full, axis=0, keepdims=True)
    e_send[...] = jnp.broadcast_to(jnp.sum(squares, axis=1, keepdims=True), e_send.shape)
    e_all[mine] = e_send[...]

    def e_copy(step):
        return remote(e_send, e_all.at[mine], e_ss.at[step - 1], e_rs.at[COUNT - step - 1], ahead(at, step))

    for step in OTHERS:
        e_copy(step).start()
    for hop in hops:
        for way in paths:
            f_copy(way, hop).wait_recv()
    new_ref[...] = p_all[...] / norm[None, None]
    for step in OTHERS:
        e_copy(step).wait_recv()
    energy_ref[...] = jnp.sum(e_all[...], axis=0)

    for way in range(len(mates)):
        quarter_copy(way).wait_send()
    for block in order:
        @pl.when((block <= z) & (z < last))
        def _():
            line_copy(block, right, r_ss).wait_send()

        @pl.when((block >= z) & (z > 0))
        def _():
            line_copy(block, left, l_ss).wait_send()

        k_copy(block).wait_send()
        for way in ways:
            d_copy(block, way).wait_send()
    for step in OTHERS:
        q_copy(step).wait_send()
        e_copy(step).wait_send()
    for way in paths:
        p_copy(way).wait_send()
        for hop in hops:
            f_copy(way, hop).wait_send()
    for hop in hops:
        n_copy(hop, z).wait_send()
    for step in range(1, spots):
        c_copy(step).wait_send()


HEIGHT_SCRATCH = 28


def second_kernel(x_hbm, t_ref, u1_ref, u2_ref, u3_ref, height_ref, new_ref, core_ref, energy_ref, z_all, *scratch):
    at = place()
    height_part(at, x_hbm, t_ref, u1_ref, u2_ref, z_all, height_ref, *scratch[:HEIGHT_SCRATCH])
    width_part(at, z_all, height_ref, u3_ref, new_ref, core_ref, energy_ref, *scratch[HEIGHT_SCRATCH:])


def second_stage(x_all, t_mat, new_time, u2, u3):
    blocks, frames, groups, _, grid_h = x_all.shape
    rank, rank_h, rank_w = new_time.shape[1], u2.shape[1], u3.shape[1]
    vmem = pl.BlockSpec(memory_space=pltpu.VMEM)
    rows = 384
    piece = rows // TILE
    width = groups * TILE
    cols = rank // TILE * PAD
    small = width // 2
    fourth = rank_w // 4

    def f32(*shape):
        return pltpu.VMEM(shape, F32)

    def bf16(*shape):
        return pltpu.VMEM(shape, BF16)

    one = pltpu.SemaphoreType.DMA
    height = [bf16(4, blocks, frames, TILE, grid_h), bf16(blocks, rank * TILE, frames * TILE),
              f32(groups, rank, TILE, grid_h), f32(groups, rank // 2, TILE, grid_h), f32(groups, rank // 4, TILE, grid_h),
              bf16(groups, rank // 4, TILE, grid_h), bf16(groups, rank // 4, TILE, grid_h),
              f32(2, rows, grid_h), f32(2, rows // 2, grid_h), f32(3, 2, piece, grid_h),
              bf16(groups, rank // 2, TILE, grid_h), f32(piece, rank_h), f32(16, piece, rank_h), one, one,
              dma(4)] + [dma(groups)] * 8 + [dma(3), dma(3), dma(COUNT), dma(16)]
    wide = [bf16(4, rank_w, 4 * width), bf16(2, 2 * PAD, grid_h), bf16(4, 2, cols, width), bf16(4, 2, cols, width), bf16(2, cols, 4 * width), bf16(4, cols, 2 * 4 * width),
            f32(4, 4 * width, 4 * width), f32(4, 2 * width, 4 * width), f32(3, 4, small, 4 * width),
            f32(4, 2 * 4, small, rank_w), f32(TILE, rank_w), f32(COUNT, TILE, rank_w),
            f32(4, 2, fourth, cols), f32(2 * 4, fourth, cols), f32(TILE, 128), f32(COUNT, TILE, 128),
            dma(3), dma(3)] + [dma(4)] * 5 + [dma(3, 4), dma(3, 4), dma(COUNT), dma(COUNT)] + [dma(7)] * 2 + [dma(7, 3)] * 2 + [dma(3)] * 2 \
        + [dma(COUNT)] * 2 + [dma(7)] * 2
    return pl.pallas_call(
        second_kernel,
        out_shape=(jax.ShapeDtypeStruct((16, piece, rank_h), F32),
                   jax.ShapeDtypeStruct((4, 2 * 4, small, rank_w), F32),
                   jax.ShapeDtypeStruct((2, fourth, cols), F32),
                   jax.ShapeDtypeStruct((TILE, 128), F32)),
        in_specs=[pl.BlockSpec(memory_space=pl.ANY), vmem, vmem, vmem, vmem],
        out_specs=(vmem, vmem, vmem, vmem),
        scratch_shapes=[bf16(2, groups, rank // 2, TILE, grid_h)] + height + wide,
        compiler_params=pltpu.CompilerParams(collective_id=2, has_side_effects=True, vmem_limit_bytes=LIMIT),
        name="second_stage",
    )(x_all, t_mat, new_time, u2.T, u3.T)


def solution(mesh):
    def local_sweep(tensor, u_time, u_height, u_width):
        frames, grid_h, grid_w = tensor.shape
        rank_t, rank_h, rank_w = u_time.shape[1], u_height.shape[1], u_width.shape[1]
        t_mat, x_all, new_time = first_stage(tensor.swapaxes(1, 2), u_width.T, u_height.T, u_time.T)
        new_time = new_time.reshape(-1, rank_t)
        power, new_width, core, energy = second_stage(x_all, t_mat, new_time, u_height, u_width)
        new_height = power.reshape(2, -1, rank_h)[:, :grid_h].reshape(-1, rank_h)
        new_width = new_width.reshape(-1, rank_w)
        core = core.reshape(2, rank_w // 4, rank_t // 8, PAD)[..., :rank_h // 2].transpose(0, 2, 3, 1)
        core_tensor = core.reshape(rank_t // 4, rank_h // 2, rank_w // 4)
        return new_time, new_height, new_width, core_tensor, energy[0, 0]

    return jax.shard_map(local_sweep, mesh=mesh, in_specs=(P("a1", "a2", "a3"), P(), P(), P()), out_specs=(P(), P(), P(), P("a1", "a2", "a3"), P()), check_vma=False)
```
